32 devices in a mesh: data: 2 (over x), expert: 16 (over z, y, core).
Axes of the slice: x: 2, y: 2, z: 4, core: 2. Of those that a mesh axis runs over, the one named last changes fastest.
Arguments:
- x_a: bfloat16 [8192, 1024], P(('data', 'expert')), parts along dimension 0
- x_b: bfloat16 [8192, 1024], P(('data', 'expert')), parts along dimension 0
- dy_b: bfloat16 [8192, 1024], P(('data', 'expert')), parts along dimension 0
- eid_a: int32 [8192, 8], P(('data', 'expert')), parts along dimension 0
- slot_a: int32 [8192, 8], P(('data', 'expert')), parts along dimension 0
- gate_a: bfloat16 [8192, 8], P(('data', 'expert')), parts along dimension 0
- eid_b: int32 [8192, 8], P(('data', 'expert')), parts along dimension 0
- slot_b: int32 [8192, 8], P(('data', 'expert')), parts along dimension 0
- gate_b: bfloat16 [8192, 8], P(('data', 'expert')), parts along dimension 0
- u_b: bfloat16 [64, 2048, 1024], P(('data', 'expert')), parts along dimension 0
- norm_1: bfloat16 [1024], replicated
- norm_2: bfloat16 [1024], replicated
- w_q: bfloat16 [1024, 16, 64], replicated
- w_k: bfloat16 [1024, 8, 64], replicated
- w_v: bfloat16 [1024, 8, 64], replicated
- w_o: bfloat16 [16, 64, 1024], replicated
- w_1: bfloat16 [32, 1024, 512], P('expert')
- w_2: bfloat16 [32, 512, 1024], P('expert')
- w_3: bfloat16 [32, 1024, 512], P('expert')
Outputs:
- output 1: bfloat16 [8192, 1024], P(('data', 'expert')), parts along dimension 0
- output 2: bfloat16 [8192, 1024], P(('data', 'expert')), parts along dimension 0
- output 3: float32 [64, 1024, 512], P(('data', 'expert')), parts along dimension 0
- output 4: float32 [64, 512, 1024], P(('data', 'expert')), parts along dimension 0
- output 5: float32 [64, 1024, 512], P(('data', 'expert')), parts along dimension 0
- output 6: float32 [32, 1024, 16, 64], P(('data', 'expert')), parts along dimension 0
- output 7: float32 [32, 1024, 8, 64], P(('data', 'expert')), parts along dimension 0
- output 8: float32 [32, 1024, 8, 64], P(('data', 'expert')), parts along dimension 0
- output 9: float32 [32, 16, 64, 1024], P(('data', 'expert')), parts along dimension 0
- output 10: float32 [32, 1024], P(('data', 'expert')), parts along dimension 0
- output 11: float32 [32, 1024], P(('data', 'expert')), parts along dimension 0
There are 2 independent parts. The reference program is written for one: setup_inputs(seed, part) draws one part's arguments, and reference() takes and returns one part's arrays. A program takes and returns all parts, laid end to end along the dimension named above; an argument that names none is the same for every part.
All inputs are finite; a program needn't handle non-finite values.
Results may differ from the reference program's by a relative error of at most 0.0176189.
Values are sent between devices in bfloat16 or wider.
A program may use at most 1 GiB of HBM per device.

```python
import jax
import jax.numpy as jnp
from jax import lax

GROUP = 16
TOKENS = 256
MODEL_DIM = 1024
HEADS = 16
KV_HEADS = 8
HEAD_DIM = 64
EXPERTS = 32
FF_DIM = 512
TOP_K = 8
ROWS = GROUP * TOKENS
CAPACITY = ((2 * TOP_K * TOKENS + 8 * EXPERTS - 1) // (8 * EXPERTS)) * 8
HOT_ROWS = min(TOKENS, CAPACITY + CAPACITY // 4)
NORM_EPS = 1e-6


def draw_routing(route_key):
    key_score, key_hot = jax.random.split(route_key, 2)
    scores = jax.random.randint(key_score, (GROUP, TOKENS, EXPERTS), 0, 2 ** 20)
    hot_ids = jax.random.randint(key_hot, (GROUP,), 0, EXPERTS)
    boosted = (jnp.arange(TOKENS)[None, :, None] < HOT_ROWS) & (jnp.arange(EXPERTS)[None, None, :] == hot_ids[:, None, None])
    scores = (scores + boosted.astype(scores.dtype) * 2 ** 20) * EXPERTS + jnp.arange(EXPERTS)
    _, expert_ids = lax.top_k(scores, TOP_K)
    flat_ids = expert_ids.reshape(GROUP, TOKENS * TOP_K)
    onehot = (flat_ids[:, :, None] == jnp.arange(EXPERTS)[None, None, :]).astype(jnp.int32)
    arrival = jnp.sum((jnp.cumsum(onehot, axis=1) - onehot) * onehot, axis=2)
    slots = jnp.where(arrival < CAPACITY, arrival, -1)
    return expert_ids.reshape(ROWS, TOP_K).astype(jnp.int32), slots.reshape(ROWS, TOP_K).astype(jnp.int32)


def slot_columns(slots):
    device_of = jnp.arange(ROWS)[:, None] // TOKENS
    return jnp.where(slots >= 0, device_of * CAPACITY + slots, GROUP * CAPACITY)


def saved_inputs(value_key, expert_ids, slots):
    filled = jnp.zeros((EXPERTS, GROUP * CAPACITY), jnp.float32).at[expert_ids, slot_columns(slots)].set(1.0, mode='drop')
    values = jax.random.normal(value_key, (EXPERTS, GROUP * CAPACITY, MODEL_DIM), jnp.float32)
    return (values * filled[:, :, None]).astype(jnp.bfloat16)


def normal_draw(draw_key, dims, scale):
    return (jax.random.normal(draw_key, dims, jnp.float32) * scale).astype(jnp.bfloat16)


def setup_inputs(seed: int = 0, part: int = 0) -> dict:
    part_key = jax.random.fold_in(jax.random.key(seed), part)
    key_list = jax.random.split(part_key, 8)
    shared = jax.random.split(jax.random.key(seed + 1), 9)
    eid_a, slot_a = draw_routing(key_list[0])
    eid_b, slot_b = draw_routing(key_list[1])
    gate_a = (jax.random.uniform(key_list[2], (ROWS, TOP_K), jnp.float32, 0.5, 1.5) / TOP_K).astype(jnp.bfloat16)
    gate_b = (jax.random.uniform(key_list[3], (ROWS, TOP_K), jnp.float32, 0.5, 1.5) / TOP_K).astype(jnp.bfloat16)
    return {
        'x_a': normal_draw(key_list[4], (ROWS, MODEL_DIM), 1.0),
        'x_b': normal_draw(key_list[5], (ROWS, MODEL_DIM), 1.0),
        'dy_b': normal_draw(key_list[6], (ROWS, MODEL_DIM), 1.0),
        'eid_a': eid_a,
        'slot_a': slot_a,
        'gate_a': gate_a,
        'eid_b': eid_b,
        'slot_b': slot_b,
        'gate_b': gate_b,
        'u_b': saved_inputs(key_list[7], eid_b, slot_b),
        'norm_1': (1.0 + 0.3 * jax.random.normal(shared[0], (MODEL_DIM,), jnp.float32)).astype(jnp.bfloat16),
        'norm_2': (1.0 + 0.3 * jax.random.normal(shared[1], (MODEL_DIM,), jnp.float32)).astype(jnp.bfloat16),
        'w_q': normal_draw(shared[2], (MODEL_DIM, HEADS, HEAD_DIM), MODEL_DIM ** -0.5),
        'w_k': normal_draw(shared[3], (MODEL_DIM, KV_HEADS, HEAD_DIM), MODEL_DIM ** -0.5),
        'w_v': normal_draw(shared[4], (MODEL_DIM, KV_HEADS, HEAD_DIM), MODEL_DIM ** -0.5),
        'w_o': normal_draw(shared[5], (HEADS, HEAD_DIM, MODEL_DIM), 2.0 * (HEADS * HEAD_DIM) ** -0.5),
        'w_1': normal_draw(shared[6], (EXPERTS, MODEL_DIM, FF_DIM), MODEL_DIM ** -0.5),
        'w_2': normal_draw(shared[7], (EXPERTS, FF_DIM, MODEL_DIM), 3.0 * FF_DIM ** -0.5),
        'w_3': normal_draw(shared[8], (EXPERTS, MODEL_DIM, FF_DIM), MODEL_DIM ** -0.5),
    }


def rms_norm(values, gain):
    wide = values.astype(jnp.float32)
    scaled = wide * lax.rsqrt(jnp.mean(wide * wide, axis=-1, keepdims=True) + NORM_EPS)
    return (scaled * gain.astype(jnp.float32)).astype(jnp.bfloat16)


def add_rows(first, second):
    return (first.astype(jnp.float32) + second.astype(jnp.float32)).astype(jnp.bfloat16)


def attn_out(x_rows, norm_gain, w_q, w_k, w_v, w_o):
    normed = rms_norm(x_rows, norm_gain).astype(jnp.float32)
    query = jnp.einsum('td,dhe->the', normed, w_q.astype(jnp.float32)).astype(jnp.bfloat16)
    query = query.reshape(TOKENS, KV_HEADS, HEADS // KV_HEADS, HEAD_DIM).astype(jnp.float32)
    key_proj = jnp.einsum('td,dge->tge', normed, w_k.astype(jnp.float32)).astype(jnp.bfloat16).astype(jnp.float32)
    val_proj = jnp.einsum('td,dge->tge', normed, w_v.astype(jnp.float32)).astype(jnp.bfloat16).astype(jnp.float32)
    scores = jnp.einsum('tgre,mge->grtm', query, key_proj) * HEAD_DIM ** -0.5
    causal = jnp.arange(TOKENS)[:, None] >= jnp.arange(TOKENS)[None, :]
    scores = jnp.where(causal, scores, -1e30)
    probs = jax.nn.softmax(scores, axis=-1).astype(jnp.bfloat16).astype(jnp.float32)
    context = jnp.einsum('grtm,mge->tgre', probs, val_proj).astype(jnp.bfloat16)
    context = context.reshape(TOKENS, HEADS, HEAD_DIM).astype(jnp.float32)
    return jnp.einsum('the,hed->td', context, w_o.astype(jnp.float32)).astype(jnp.bfloat16)


def expert_forward(buf, w_1, w_2, w_3):
    act_1 = jnp.dot(buf, w_1, preferred_element_type=jnp.float32).astype(jnp.bfloat16).astype(jnp.float32)
    act_3 = jnp.dot(buf, w_3, preferred_element_type=jnp.float32).astype(jnp.bfloat16).astype(jnp.float32)
    hidden = (act_1 * jax.nn.sigmoid(act_1) * act_3).astype(jnp.bfloat16)
    return jnp.dot(hidden, w_2, preferred_element_type=jnp.float32).astype(jnp.bfloat16)


def expert_backward(saved, d_out, w_1, w_2, w_3):
    pre_1 = jnp.dot(saved, w_1, preferred_element_type=jnp.float32).astype(jnp.bfloat16).astype(jnp.float32)
    pre_3 = jnp.dot(saved, w_3, preferred_element_type=jnp.float32).astype(jnp.bfloat16).astype(jnp.float32)
    sigma = jax.nn.sigmoid(pre_1)
    silu_1 = pre_1 * sigma
    hidden = (silu_1 * pre_3).astype(jnp.bfloat16)
    grad_w2 = jnp.dot(hidden.T, d_out, preferred_element_type=jnp.float32)
    grad_hid = jnp.dot(d_out, w_2.T, preferred_element_type=jnp.float32).astype(jnp.bfloat16).astype(jnp.float32)
    grad_a1 = (grad_hid * pre_3 * sigma * (1.0 + pre_1 * (1.0 - sigma))).astype(jnp.bfloat16)
    grad_a3 = (grad_hid * silu_1).astype(jnp.bfloat16)
    grad_w1 = jnp.dot(saved.T, grad_a1, preferred_element_type=jnp.float32)
    grad_w3 = jnp.dot(saved.T, grad_a3, preferred_element_type=jnp.float32)
    grad_in = (jnp.dot(grad_a1, w_1.T, preferred_element_type=jnp.float32) + jnp.dot(grad_a3, w_3.T, preferred_element_type=jnp.float32)).astype(jnp.bfloat16)
    return grad_w1, grad_w2, grad_w3, grad_in


def pick_rows(buf, expert_ids, columns):
    padded = jnp.concatenate([buf, jnp.zeros((EXPERTS, 1, MODEL_DIM), buf.dtype)], axis=1)
    return padded[expert_ids, columns]


def reference(x_a, x_b, dy_b, eid_a, slot_a, gate_a, eid_b, slot_b, gate_b, u_b, norm_1, norm_2, w_q, w_k, w_v, w_o, w_1, w_2, w_3):
    def forward_rows(x_dev):
        return add_rows(x_dev, attn_out(x_dev, norm_1, w_q, w_k, w_v, w_o))
    h_a = lax.map(forward_rows, x_a.reshape(GROUP, TOKENS, MODEL_DIM)).reshape(ROWS, MODEL_DIM)
    u_a = rms_norm(h_a, norm_2)
    cols_a = slot_columns(slot_a)
    buf_a = jnp.zeros((EXPERTS, GROUP * CAPACITY, MODEL_DIM), jnp.bfloat16).at[eid_a, cols_a].set(jnp.broadcast_to(u_a[:, None, :], (ROWS, TOP_K, MODEL_DIM)), mode='drop')
    out_a = lax.map(lambda item: expert_forward(item[0], item[1], item[2], item[3]), (buf_a, w_1, w_2, w_3))
    picked = pick_rows(out_a, eid_a, cols_a).astype(jnp.float32)
    mixed = jnp.sum(gate_a.astype(jnp.float32)[:, :, None] * picked, axis=1)
    y_a = (h_a.astype(jnp.float32) + mixed).astype(jnp.bfloat16)
    cols_b = slot_columns(slot_b)
    grad_rows = (gate_b.astype(jnp.float32)[:, :, None] * dy_b.astype(jnp.float32)[:, None, :]).astype(jnp.bfloat16)
    d_out = jnp.zeros((EXPERTS, GROUP * CAPACITY, MODEL_DIM), jnp.bfloat16).at[eid_b, cols_b].set(grad_rows, mode='drop')
    grad_w1, grad_w2, grad_w3, grad_in = lax.map(lambda item: expert_backward(item[0], item[1], item[2], item[3], item[4]), (u_b, d_out, w_1, w_2, w_3))
    du_rows = jnp.sum(pick_rows(grad_in, eid_b, cols_b).astype(jnp.float32), axis=1).astype(jnp.bfloat16)
    def backward_rows(item):
        x_dev, dy_dev, du_dev = item
        attn_val, attn_pull = jax.vjp(attn_out, x_dev, norm_1, w_q, w_k, w_v, w_o)
        h_dev = add_rows(x_dev, attn_val)
        _, norm_pull = jax.vjp(rms_norm, h_dev, norm_2)
        dh_norm, grad_n2 = norm_pull(du_dev)
        dh_dev = add_rows(dy_dev, dh_norm)
        grad_x, grad_n1, grad_q, grad_k, grad_v, grad_o = attn_pull(dh_dev)
        return (add_rows(dh_dev, grad_x), grad_q.astype(jnp.float32), grad_k.astype(jnp.float32), grad_v.astype(jnp.float32), grad_o.astype(jnp.float32), grad_n1.astype(jnp.float32), grad_n2.astype(jnp.float32))
    dx_b, g_q, g_k, g_v, g_o, g_n1, g_n2 = lax.map(backward_rows, (x_b.reshape(GROUP, TOKENS, MODEL_DIM), dy_b.reshape(GROUP, TOKENS, MODEL_DIM), du_rows.reshape(GROUP, TOKENS, MODEL_DIM)))
    return (y_a, dx_b.reshape(ROWS, MODEL_DIM), grad_w1, grad_w2, grad_w3, g_q, g_k, g_v, g_o, g_n1, g_n2)
```

```python
import jax
import jax.numpy as jnp
from jax import lax
from jax.sharding import PartitionSpec as P

NORM_EPS = 1e-6


def rms_norm(values, gain):
    wide = values.astype(jnp.float32)
    scaled = wide * lax.rsqrt(jnp.mean(wide * wide, axis=-1, keepdims=True) + NORM_EPS)
    return (scaled * gain.astype(jnp.float32)).astype(jnp.bfloat16)


def add_rows(first, second):
    return (first.astype(jnp.float32) + second.astype(jnp.float32)).astype(jnp.bfloat16)


def attn_out(x_rows, norm_gain, w_q, w_k, w_v, w_o):
    tokens = x_rows.shape[0]
    heads = w_q.shape[1]
    kv_heads = w_k.shape[1]
    head_dim = w_q.shape[2]
    normed = rms_norm(x_rows, norm_gain)
    query = jnp.einsum('td,dhe->the', normed, w_q, preferred_element_type=jnp.float32).astype(jnp.bfloat16)
    query = query.reshape(tokens, kv_heads, heads // kv_heads, head_dim)
    key_proj = jnp.einsum('td,dge->tge', normed, w_k, preferred_element_type=jnp.float32).astype(jnp.bfloat16)
    val_proj = jnp.einsum('td,dge->tge', normed, w_v, preferred_element_type=jnp.float32).astype(jnp.bfloat16)
    scores = jnp.einsum('tgre,mge->grtm', query, key_proj, preferred_element_type=jnp.float32) * head_dim ** -0.5
    causal = jnp.arange(tokens)[:, None] >= jnp.arange(tokens)[None, :]
    scores = jnp.where(causal, scores, -1e30)
    probs = jax.nn.softmax(scores, axis=-1).astype(jnp.bfloat16)
    context = jnp.einsum('grtm,mge->tgre', probs, val_proj, preferred_element_type=jnp.float32).astype(jnp.bfloat16)
    context = context.reshape(tokens, heads, head_dim)
    return jnp.einsum('the,hed->td', context, w_o, preferred_element_type=jnp.float32).astype(jnp.bfloat16)


def routing_table(expert_ids, slot_ids, gates, experts):
    hit = (expert_ids[:, :, None] == jnp.arange(experts)[None, None, :]) & (slot_ids >= 0)[:, :, None]
    slots = jnp.sum(jnp.where(hit, slot_ids[:, :, None] + 1, 0), axis=1) - 1
    weights = jnp.sum(jnp.where(hit, gates.astype(jnp.float32)[:, :, None], 0.0), axis=1)
    return slots.astype(jnp.bfloat16), weights.astype(jnp.bfloat16)


def device_backward(x_dev, dy_dev, du_dev, norm_1, norm_2, w_q, w_k, w_v, w_o):
    attn_val, attn_pull = jax.vjp(attn_out, x_dev, norm_1, w_q, w_k, w_v, w_o)
    h_dev = add_rows(x_dev, attn_val)
    _, norm_pull = jax.vjp(rms_norm, h_dev, norm_2)
    dh_norm, grad_n2 = norm_pull(du_dev)
    dh_dev = add_rows(dy_dev, dh_norm)
    grad_x, grad_n1, grad_q, grad_k, grad_v, grad_o = attn_pull(dh_dev)
    return (add_rows(dh_dev, grad_x), grad_q.astype(jnp.float32), grad_k.astype(jnp.float32), grad_v.astype(jnp.float32), grad_o.astype(jnp.float32), grad_n1.astype(jnp.float32), grad_n2.astype(jnp.float32))


def solution(mesh):
    group = mesh.shape['expert']

    def local_step(x_a, x_b, dy_b, eid_a, slot_a, gate_a, eid_b, slot_b, gate_b, u_b, norm_1, norm_2, w_q, w_k, w_v, w_o, w_1, w_2, w_3):
        local_experts = w_1.shape[0]
        experts = local_experts * group
        capacity = u_b.shape[1] // group
        model_dim = x_a.shape[1]

        tokens = x_a.shape[0]
        me = lax.axis_index('expert')
        meta = jnp.concatenate(routing_table(eid_b, slot_b, gate_b, experts) + routing_table(eid_a, slot_a, gate_a, experts), axis=1)
        meta_all = lax.all_gather(meta, 'expert', axis=0)
        dy_all = lax.all_gather(dy_b, 'expert', axis=0)
        h_a = add_rows(x_a, attn_out(x_a, norm_1, w_q, w_k, w_v, w_o))
        u_a = rms_norm(h_a, norm_2)
        u_all = lax.all_gather(u_a, 'expert', axis=0)

        fields = meta_all.reshape(group, tokens, 4, group, local_experts)
        mine = lax.dynamic_index_in_dim(fields, me, 3, keepdims=False)
        slot_of_b, gate_of_b, slot_of_a, gate_of_a = mine[:, :, 0], mine[:, :, 1], mine[:, :, 2], mine[:, :, 3]
        columns = jnp.arange(capacity).astype(jnp.bfloat16)

        def place(slots, weights):
            return jnp.where(slots[:, :, :, None] == columns, weights[:, :, :, None], jnp.zeros((), jnp.bfloat16))

        ones = jnp.ones_like(gate_of_b)
        gated_b = place(slot_of_b, gate_of_b)
        plain_b = place(slot_of_b, ones)
        gated_a = place(slot_of_a, gate_of_a)
        plain_a = place(slot_of_a, ones)

        saved = u_b.reshape(local_experts, group, capacity, model_dim)
        pre_1 = jnp.einsum('epcd,edf->epcf', saved, w_1, preferred_element_type=jnp.float32).astype(jnp.bfloat16).astype(jnp.float32)
        pre_3 = jnp.einsum('epcd,edf->epcf', saved, w_3, preferred_element_type=jnp.float32).astype(jnp.bfloat16).astype(jnp.float32)
        sigma = jax.nn.sigmoid(pre_1)
        silu_1 = pre_1 * sigma
        hid_b = (silu_1 * pre_3).astype(jnp.bfloat16)
        d_out = jnp.einsum('ptec,ptd->epcd', gated_b, dy_all, preferred_element_type=jnp.float32).astype(jnp.bfloat16)
        grad_hid = jnp.einsum('epcd,efd->epcf', d_out, w_2, preferred_element_type=jnp.float32).astype(jnp.bfloat16).astype(jnp.float32)
        grad_a1 = (grad_hid * pre_3 * sigma * (1.0 + pre_1 * (1.0 - sigma))).astype(jnp.bfloat16)
        grad_a3 = (grad_hid * silu_1).astype(jnp.bfloat16)
        grad_in = (jnp.einsum('epcf,edf->epcd', grad_a1, w_1, preferred_element_type=jnp.float32) + jnp.einsum('epcf,edf->epcd', grad_a3, w_3, preferred_element_type=jnp.float32)).astype(jnp.bfloat16)
        part_b = jnp.einsum('ptec,epcd->ptd', plain_b, grad_in, preferred_element_type=jnp.float32).reshape(group * tokens, model_dim)
        du_rows = lax.psum_scatter(part_b, 'expert', scatter_dimension=0, tiled=True).astype(jnp.bfloat16)
        grad_w2 = jnp.einsum('epcf,epcd->efd', hid_b, d_out, preferred_element_type=jnp.float32)
        grad_w1 = jnp.einsum('epcd,epcf->edf', saved, grad_a1, preferred_element_type=jnp.float32)
        grad_w3 = jnp.einsum('epcd,epcf->edf', saved, grad_a3, preferred_element_type=jnp.float32)

        recv_a = jnp.einsum('ptec,ptd->epcd', plain_a, u_all, preferred_element_type=jnp.float32).astype(jnp.bfloat16)
        act_1 = jnp.einsum('epcd,edf->epcf', recv_a, w_1, preferred_element_type=jnp.float32).astype(jnp.bfloat16).astype(jnp.float32)
        act_3 = jnp.einsum('epcd,edf->epcf', recv_a, w_3, preferred_element_type=jnp.float32).astype(jnp.bfloat16).astype(jnp.float32)
        hidden = (act_1 * jax.nn.sigmoid(act_1) * act_3).astype(jnp.bfloat16)
        out_a = jnp.einsum('epcf,efd->epcd', hidden, w_2, preferred_element_type=jnp.float32).astype(jnp.bfloat16)
        part_a = jnp.einsum('ptec,epcd->ptd', gated_a, out_a, preferred_element_type=jnp.float32).reshape(group * tokens, model_dim)
        mixed = lax.psum_scatter(part_a, 'expert', scatter_dimension=0, tiled=True)
        y_a = (h_a.astype(jnp.float32) + mixed).astype(jnp.bfloat16)

        dx_b, g_q, g_k, g_v, g_o, g_n1, g_n2 = device_backward(x_b, dy_b, du_rows, norm_1, norm_2, w_q, w_k, w_v, w_o)
        return (y_a, dx_b, grad_w1, grad_w2, grad_w3, g_q[None], g_k[None], g_v[None], g_o[None], g_n1[None], g_n2[None])

    row_spec = P(('data', 'expert'), None)
    cube_spec = P(('data', 'expert'), None, None)
    quad_spec = P(('data', 'expert'), None, None, None)
    expert_spec = P('expert', None, None)
    in_specs = (row_spec, row_spec, row_spec, row_spec, row_spec, row_spec, row_spec, row_spec, row_spec, cube_spec, P(), P(), P(), P(), P(), P(), expert_spec, expert_spec, expert_spec)
    out_specs = (row_spec, row_spec, cube_spec, cube_spec, cube_spec, quad_spec, quad_spec, quad_spec, quad_spec, row_spec, row_spec)
    return jax.shard_map(local_step, mesh=mesh, in_specs=in_specs, out_specs=out_specs, check_vma=False)
```

```python
import functools

import jax
import jax.numpy as jnp
from jax import lax
from jax.experimental import pallas as pl
from jax.experimental.pallas import tpu as pltpu
from jax.sharding import PartitionSpec as P

F32 = jnp.float32
BF16 = jnp.bfloat16
VMEM_BYTES = 66_000_000

NORM_EPS = 1e-6


def rms_norm(values, gain):
    wide = values.astype(jnp.float32)
    scaled = wide * lax.rsqrt(jnp.mean(wide * wide, axis=-1, keepdims=True) + NORM_EPS)
    return (scaled * gain.astype(jnp.float32)).astype(jnp.bfloat16)


def add_rows(first, second):
    return (first.astype(jnp.float32) + second.astype(jnp.float32)).astype(jnp.bfloat16)


def attn_out(x_rows, norm_gain, w_q, w_k, w_v, w_o):
    tokens = x_rows.shape[0]
    heads = w_q.shape[1]
    kv_heads = w_k.shape[1]
    head_dim = w_q.shape[2]
    normed = rms_norm(x_rows, norm_gain)
    query = jnp.einsum('td,dhe->the', normed, w_q, preferred_element_type=jnp.float32).astype(jnp.bfloat16)
    query = query.reshape(tokens, kv_heads, heads // kv_heads, head_dim)
    key_proj = jnp.einsum('td,dge->tge', normed, w_k, preferred_element_type=jnp.float32).astype(jnp.bfloat16)
    val_proj = jnp.einsum('td,dge->tge', normed, w_v, preferred_element_type=jnp.float32).astype(jnp.bfloat16)
    scores = jnp.einsum('tgre,mge->grtm', query, key_proj, preferred_element_type=jnp.float32) * head_dim ** -0.5
    causal = jnp.arange(tokens)[:, None] >= jnp.arange(tokens)[None, :]
    scores = jnp.where(causal, scores, -1e30)
    probs = jax.nn.softmax(scores, axis=-1).astype(jnp.bfloat16)
    context = jnp.einsum('grtm,mge->tgre', probs, val_proj, preferred_element_type=jnp.float32).astype(jnp.bfloat16)
    context = context.reshape(tokens, heads, head_dim)
    return jnp.einsum('the,hed->td', context, w_o, preferred_element_type=jnp.float32).astype(jnp.bfloat16)


def routing_table(expert_ids, slot_ids, gates, experts):
    hit = (expert_ids[:, :, None] == jnp.arange(experts)[None, None, :]) & (slot_ids >= 0)[:, :, None]
    slots = jnp.sum(jnp.where(hit, slot_ids[:, :, None] + 1, 0), axis=1) - 1
    weights = jnp.sum(jnp.where(hit, gates.astype(jnp.float32)[:, :, None], 0.0), axis=1)
    return slots.astype(jnp.bfloat16), weights.astype(jnp.bfloat16)


def mm(left, right):
    return lax.dot_general(left, right, (((1,), (0,)), ((), ())), preferred_element_type=F32)


def mm_nt(left, right):
    return lax.dot_general(left, right, (((1,), (1,)), ((), ())), preferred_element_type=F32)


def mm_tn(left, right):
    return lax.dot_general(left, right, (((0,), (0,)), ((), ())), preferred_element_type=F32)


def exchange_kernel(backward, *refs):
    if backward:
        (rows_ref, u_ref, w1_ref, w3_ref, w2_ref, out_ref, gw1_ref, gw2_ref, gw3_ref,
         got, own, stage, from_core, from_y, from_z, saved, acc1, acc2, acc3,
         own_sem, load_sem, store_sem, g_recv, g_core, g_y, g_z, s_core, r_core, s_y, r_y, s_z, r_z) = refs
    else:
        (rows_ref, w1_ref, w3_ref, w2_ref, out_ref,
         got, own, stage, from_core, from_y, from_z,
         own_sem, g_recv, g_core, g_y, g_z, s_core, r_core, s_y, r_y, s_z, r_z) = refs
    tokens, dim = own.shape[1], own.shape[2]
    half = w1_ref.shape[0]
    me = lax.axis_index('expert')
    z, y, c = lax.div(me, 4), lax.rem(lax.div(me, 2), 2), lax.rem(me, 2)

    def at(zz, yy, cc):
        return (zz * 2 + yy) * 2 + cc

    other_core = at(z, y, 1 - c)
    other_y = at(z, 1 - y, c)

    def z_peer(k):
        return at(lax.rem(z + k, 4), y, c)

    def remote(src, dst, send, recv, peer):
        return pltpu.make_async_remote_copy(src_ref=src, dst_ref=dst, send_sem=send, recv_sem=recv, device_id={'expert': peer}, device_id_type=pl.DeviceIdType.MESH)

    barrier = pltpu.get_barrier_semaphore()
    for peer in (other_core, other_y, z_peer(1), z_peer(2), z_peer(3)):
        pl.semaphore_signal(barrier, inc=1, device_id={'expert': peer}, device_id_type=pl.DeviceIdType.MESH)
    load_own = pltpu.make_async_copy(rows_ref, got.at[me], own_sem)
    load_own.start()
    pl.semaphore_wait(barrier, 5)
    load_own.wait()

    def gather_to_core(slot, block):
        return remote(got.at[block], got.at[block], g_core.at[slot], g_recv.at[block], other_core)

    def gather_to_y(k, block):
        return remote(got.at[block], got.at[block], g_y.at[k], g_recv.at[block], other_y)

    def gather_to_z(k):
        return remote(got.at[me], got.at[me], g_z.at[k - 1], g_recv.at[me], z_peer(k))

    def arrived(block):
        remote(got.at[block], got.at[block], g_core.at[0], g_recv.at[block], other_core).wait_recv()

    gather_to_y(0, me).start()
    for k in (2, 1, 3):
        gather_to_z(k).start()
    gather_to_core(0, me).start()

    def forward_z(k):
        block = at(lax.rem(z + k, 4), y, c)
        arrived(block)
        gather_to_y(k, block).start()
        gather_to_core(k, block).start()

    def order(step):
        i = lax.div(step + 1, 2)
        k = lax.rem(2 * i + lax.rem(lax.div(i, 2), 2), 4)
        across = lax.rem(step + 1, 2) * lax.div(step + 7, 8) + lax.div(step, 7)
        return k, across

    def pair_base(step):
        k, across = order(step)
        return at(lax.rem(z + k, 4), lax.rem(y + across, 2), 0)

    if backward:
        slots = saved.shape[2] // 2

        def load_saved(step):
            start = pl.multiple_of(pair_base(step) * slots, 2 * slots)
            which = lax.rem(step, 2)
            return pltpu.make_async_copy(u_ref.at[:, pl.ds(start, 2 * slots), :], saved.at[which], load_sem.at[which])

        load_saved(0).start()
        acc1[...] = jnp.zeros_like(acc1)
        acc2[...] = jnp.zeros_like(acc2)
        acc3[...] = jnp.zeros_like(acc3)
    else:
        slots = tokens // 2

    sel = (lax.broadcasted_iota(jnp.int32, (16, 16), 1) == me).astype(BF16)
    slot_row = lax.broadcasted_iota(jnp.int32, (slots, tokens), 0).astype(F32)

    def masks(block):
        table = mm(sel, got[block, tokens:, :])
        plain, gated = [], []
        for e in range(half):
            hit = table[0:1, e * tokens:(e + 1) * tokens] == slot_row
            gate = table[0:1, (half + e) * tokens:(half + e + 1) * tokens]
            plain.append(jnp.where(hit, 1.0, 0.0).astype(BF16))
            gated.append(jnp.where(hit, gate, 0.0).astype(BF16))
        return jnp.concatenate(plain, axis=0), jnp.concatenate(gated, axis=0)

    def experts_forward(mine, theirs):
        marks = [masks(block) for block in (mine, theirs)]
        placed = [mm(marks[s][0], got[block, :tokens, :]).astype(BF16) for s, block in enumerate((mine, theirs))]
        outs = []
        for e in range(half):
            rows = jnp.concatenate([part[e * slots:(e + 1) * slots] for part in placed], axis=0)
            act_1 = mm(rows, w1_ref[e]).astype(BF16).astype(F32)
            act_3 = mm(rows, w3_ref[e]).astype(BF16).astype(F32)
            hidden = (act_1 * jax.nn.sigmoid(act_1) * act_3).astype(BF16)
            outs.append(mm(hidden, w2_ref[e]).astype(BF16))

        def combine(s):
            return mm_tn(marks[s][1], jnp.concatenate([out[s * slots:(s + 1) * slots] for out in outs], axis=0))

        return combine

    def experts_backward(mine, theirs, which):
        marks = [masks(block) for block in (mine, theirs)]
        placed = [mm(marks[s][1], got[block, :tokens, :]).astype(BF16) for s, block in enumerate((mine, theirs))]
        outs = []
        for e in range(half):
            rows = saved[which, e]
            d_out = jnp.concatenate([part[e * slots:(e + 1) * slots] for part in placed], axis=0)
            pre_1 = mm(rows, w1_ref[e]).astype(BF16).astype(F32)
            pre_3 = mm(rows, w3_ref[e]).astype(BF16).astype(F32)
            sigma = jax.nn.sigmoid(pre_1)
            silu_1 = pre_1 * sigma
            hidden = (silu_1 * pre_3).astype(BF16)
            acc2[e] += mm_tn(hidden, d_out)
            grad_hid = mm_nt(d_out, w2_ref[e]).astype(BF16).astype(F32)
            grad_a1 = (grad_hid * pre_3 * sigma * (1.0 + pre_1 * (1.0 - sigma))).astype(BF16)
            grad_a3 = (grad_hid * silu_1).astype(BF16)
            acc1[e] += mm_tn(rows, grad_a1)
            acc3[e] += mm_tn(rows, grad_a3)
            outs.append((mm_nt(grad_a1, w1_ref[e]) + mm_nt(grad_a3, w3_ref[e])).astype(BF16))

        def combine(s):
            return mm_tn(marks[s][0], jnp.concatenate([out[s * slots:(s + 1) * slots] for out in outs], axis=0))

        return combine

    def send_core(step):
        which = lax.rem(step, 2)
        return remote(stage.at[which], from_core.at[which], s_core.at[which], r_core.at[which], other_core)

    def send_y(k):
        return remote(own.at[4 + k], from_y.at[k], s_y.at[k], r_y.at[k], other_y)

    def send_z(k):
        return remote(own.at[k], from_z.at[k - 1], s_z.at[k - 1], r_z.at[k - 1], z_peer(k))

    def take_y(k):
        send_y(k).wait_recv()
        own[k] += from_y[k]

    def step_body(step, carry):
        k, across = order(step)
        base = pair_base(step)
        which = lax.rem(step, 2)

        @pl.when(step == 1)
        def _():
            forward_z(2)

        @pl.when(across == 1)
        def _():
            arrived(base + c)
            gather_to_core(4 + k, base + c).start()

        arrived(base + 1 - c)
        if backward:
            @pl.when(step < 7)
            def _():
                load_saved(step + 1).start()
            load_saved(step).wait()
            low, high = base, base + 1
            combine = experts_backward(low, high, which)
        else:
            low, high = base, base + 1
            combine = experts_forward(low, high)

        @pl.when(step >= 2)
        def _():
            send_core(step).wait_send()

        first, second = combine(0), combine(1)

        @pl.when(c == 0)
        def _():
            stage[which] = second
            own[across * 4 + k] = first

        @pl.when(c == 1)
        def _():
            stage[which] = first
            own[across * 4 + k] = second

        send_core(step).start()

        @pl.when(step == 1)
        def _():
            forward_z(1)

        @pl.when(step == 2)
        def _():
            forward_z(3)

        send_core(step).wait_recv()
        own[across * 4 + k] += from_core[which]

        @pl.when(across == 1)
        def _():
            send_y(k).start()

        @pl.when(step == 5)
        def _():
            take_y(2)
            send_z(2).start()

        return carry

    lax.fori_loop(0, 8, step_body, 0)
    if backward:
        stores = [pltpu.make_async_copy(acc, ref, store_sem.at[i]) for i, (acc, ref) in enumerate(((acc1, gw1_ref), (acc2, gw2_ref), (acc3, gw3_ref)))]
        for store in stores:
            store.start()
    for k in (1, 3):
        take_y(k)
        send_z(k).start()
    take_y(0)
    for k in (2, 1, 3):
        send_z(k).wait_recv()
    out_ref[...] = (own[0] + from_z[0] + (from_z[1] + from_z[2])).astype(out_ref.dtype)
    for k in (1, 2, 3):
        send_z(k).wait_send()
        gather_to_z(k).wait_send()
    for k in range(4):
        send_y(k).wait_send()
        gather_to_y(k, me).wait_send()
    for slot in range(8):
        gather_to_core(slot, me).wait_send()
    send_core(0).wait_send()
    send_core(1).wait_send()
    if backward:
        for store in stores:
            store.wait()


def exchange(backward, rows, weights, tokens, saved=None):
    w_1, w_3, w_2 = weights
    dim = rows.shape[1]
    half, ff = w_1.shape[0], w_1.shape[2]
    dma = pltpu.SemaphoreType.DMA
    block = (tokens, dim)
    scratch = [
        pltpu.VMEM((16,) + rows.shape, BF16),
        pltpu.VMEM((8,) + block, F32),
        pltpu.VMEM((2,) + block, F32),
        pltpu.VMEM((2,) + block, F32),
        pltpu.VMEM((4,) + block, F32),
        pltpu.VMEM((3,) + block, F32),
    ]
    tail = [dma((16,)), dma((8,)), dma((4,)), dma((3,)), dma((2,)), dma((2,)), dma((4,)), dma((4,)), dma((3,)), dma((3,))]
    any_spec = pl.BlockSpec(memory_space=pl.ANY)
    vmem_spec = pl.BlockSpec(memory_space=pltpu.VMEM)
    if backward:
        slots = saved.shape[1] // 16
        scratch += [
            pltpu.VMEM((2, half, 2 * slots, dim), BF16),
            pltpu.VMEM((half, dim, ff), F32),
            pltpu.VMEM((half, ff, dim), F32),
            pltpu.VMEM((half, dim, ff), F32),
            dma(()), dma((2,)), dma((3,)),
        ]
        operands = (rows, saved, w_1, w_3, w_2)
        in_specs = [any_spec, any_spec, vmem_spec, vmem_spec, vmem_spec]
        out_shape = [jax.ShapeDtypeStruct(block, BF16), jax.ShapeDtypeStruct((half, dim, ff), F32), jax.ShapeDtypeStruct((half, ff, dim), F32), jax.ShapeDtypeStruct((half, dim, ff), F32)]
        out_specs = [vmem_spec, any_spec, any_spec, any_spec]
    else:
        scratch += [dma(())]
        operands = (rows, w_1, w_3, w_2)
        in_specs = [any_spec, vmem_spec, vmem_spec, vmem_spec]
        out_shape = [jax.ShapeDtypeStruct(block, F32)]
        out_specs = [vmem_spec]
    return pl.pallas_call(
        functools.partial(exchange_kernel, backward),
        out_shape=out_shape,
        in_specs=in_specs,
        out_specs=out_specs,
        scratch_shapes=scratch + tail,
        name='exchange_b' if backward else 'exchange_a',
        compiler_params=pltpu.CompilerParams(collective_id=1 if backward else 0, has_side_effects=True, vmem_limit_bytes=VMEM_BYTES),
    )(*operands)


def device_backward(x_dev, dy_dev, du_dev, norm_1, norm_2, w_q, w_k, w_v, w_o):
    attn_val, attn_pull = jax.vjp(attn_out, x_dev, norm_1, w_q, w_k, w_v, w_o)
    h_dev = add_rows(x_dev, attn_val)
    _, norm_pull = jax.vjp(rms_norm, h_dev, norm_2)
    dh_norm, grad_n2 = norm_pull(du_dev)
    dh_dev = add_rows(dy_dev, dh_norm)
    grad_x, grad_n1, grad_q, grad_k, grad_v, grad_o = attn_pull(dh_dev)
    return (add_rows(dh_dev, grad_x), grad_q.astype(jnp.float32), grad_k.astype(jnp.float32), grad_v.astype(jnp.float32), grad_o.astype(jnp.float32), grad_n1.astype(jnp.float32), grad_n2.astype(jnp.float32))


def solution(mesh):
    group = mesh.shape['expert']

    def local_step(x_a, x_b, dy_b, eid_a, slot_a, gate_a, eid_b, slot_b, gate_b, u_b, norm_1, norm_2, w_q, w_k, w_v, w_o, w_1, w_2, w_3):
        local_experts = w_1.shape[0]
        experts = local_experts * group
        model_dim = x_a.shape[1]

        tokens = x_a.shape[0]

        def with_routing(rows, expert_ids, slot_ids, gates):
            slots, weights = routing_table(expert_ids, slot_ids, gates, experts)
            table = jnp.stack([slots, weights], axis=1).reshape(tokens, 2, group, local_experts)
            table = table.transpose(2, 1, 3, 0).reshape(group, 2 * local_experts * tokens)
            table = jnp.pad(table, ((0, 0), (0, model_dim - table.shape[1])))
            return jnp.concatenate([rows, table], axis=0)

        weights = (w_1, w_3, w_2)
        du_rows, grad_w1, grad_w2, grad_w3 = exchange(True, with_routing(dy_b, eid_b, slot_b, gate_b), weights, tokens, u_b)
        h_a = add_rows(x_a, attn_out(x_a, norm_1, w_q, w_k, w_v, w_o))
        u_a = rms_norm(h_a, norm_2)
        mixed = exchange(False, with_routing(u_a, eid_a, slot_a, gate_a), weights, tokens)[0]
        y_a = (h_a.astype(jnp.float32) + mixed).astype(jnp.bfloat16)
        dx_b, g_q, g_k, g_v, g_o, g_n1, g_n2 = device_backward(x_b, dy_b, du_rows, norm_1, norm_2, w_q, w_k, w_v, w_o)
        return (y_a, dx_b, grad_w1, grad_w2, grad_w3, g_q[None], g_k[None], g_v[None], g_o[None], g_n1[None], g_n2[None])

    row_spec = P(('data', 'expert'), None)
    cube_spec = P(('data', 'expert'), None, None)
    quad_spec = P(('data', 'expert'), None, None, None)
    expert_spec = P('expert', None, None)
    in_specs = (row_spec, row_spec, row_spec, row_spec, row_spec, row_spec, row_spec, row_spec, row_spec, cube_spec, P(), P(), P(), P(), P(), P(), expert_spec, expert_spec, expert_spec)
    out_specs = (row_spec, row_spec, cube_spec, cube_spec, cube_spec, quad_spec, quad_spec, quad_spec, quad_spec, row_spec, row_spec)
    return jax.shard_map(local_step, mesh=mesh, in_specs=in_specs, out_specs=out_specs, check_vma=False)
```

```python
import functools

import jax
import jax.numpy as jnp
from jax import lax
from jax.experimental import pallas as pl
from jax.experimental.pallas import tpu as pltpu
from jax.sharding import PartitionSpec as P

F32 = jnp.float32
BF16 = jnp.bfloat16
VMEM_BYTES = 66_000_000

NORM_EPS = 1e-6


def rms_norm(values, gain):
    wide = values.astype(jnp.float32)
    scaled = wide * lax.rsqrt(jnp.mean(wide * wide, axis=-1, keepdims=True) + NORM_EPS)
    return (scaled * gain.astype(jnp.float32)).astype(jnp.bfloat16)


def add_rows(first, second):
    return (first.astype(jnp.float32) + second.astype(jnp.float32)).astype(jnp.bfloat16)


def attn_out(x_rows, norm_gain, w_q, w_k, w_v, w_o):
    tokens = x_rows.shape[0]
    heads = w_q.shape[1]
    kv_heads = w_k.shape[1]
    head_dim = w_q.shape[2]
    normed = rms_norm(x_rows, norm_gain)
    query = jnp.einsum('td,dhe->the', normed, w_q, preferred_element_type=jnp.float32).astype(jnp.bfloat16)
    query = query.reshape(tokens, kv_heads, heads // kv_heads, head_dim)
    key_proj = jnp.einsum('td,dge->tge', normed, w_k, preferred_element_type=jnp.float32).astype(jnp.bfloat16)
    val_proj = jnp.einsum('td,dge->tge', normed, w_v, preferred_element_type=jnp.float32).astype(jnp.bfloat16)
    scores = jnp.einsum('tgre,mge->grtm', query, key_proj, preferred_element_type=jnp.float32) * head_dim ** -0.5
    causal = jnp.arange(tokens)[:, None] >= jnp.arange(tokens)[None, :]
    scores = jnp.where(causal, scores, -1e30)
    probs = jax.nn.softmax(scores, axis=-1).astype(jnp.bfloat16)
    context = jnp.einsum('grtm,mge->tgre', probs, val_proj, preferred_element_type=jnp.float32).astype(jnp.bfloat16)
    context = context.reshape(tokens, heads, head_dim)
    return jnp.einsum('the,hed->td', context, w_o, preferred_element_type=jnp.float32).astype(jnp.bfloat16)


def routing_table(expert_ids, slot_ids, gates, experts):
    hit = (expert_ids[:, :, None] == jnp.arange(experts)[None, None, :]) & (slot_ids >= 0)[:, :, None]
    slots = jnp.sum(jnp.where(hit, slot_ids[:, :, None] + 1, 0), axis=1) - 1
    weights = jnp.sum(jnp.where(hit, gates.astype(jnp.float32)[:, :, None], 0.0), axis=1)
    return slots.astype(jnp.bfloat16), weights.astype(jnp.bfloat16)


def mm(left, right):
    return lax.dot_general(left, right, (((1,), (0,)), ((), ())), preferred_element_type=F32)


def mm_nt(left, right):
    return lax.dot_general(left, right, (((1,), (1,)), ((), ())), preferred_element_type=F32)


def mm_tn(left, right):
    return lax.dot_general(left, right, (((0,), (0,)), ((), ())), preferred_element_type=F32)


def exchange_kernel(backward, *refs):
    if backward:
        (rows_ref, u_ref, w1_ref, w3_ref, w2_ref, out_ref, gw1_ref, gw2_ref, gw3_ref,
         got, own, stage, from_core, from_y, from_z, saved, acc1, acc2, acc3,
         own_sem, load_sem, store_sem, g_recv, g_core, g_y, g_z, s_core, r_core, s_y, r_y, s_z, r_z) = refs
    else:
        (rows_ref, w1_ref, w3_ref, w2_ref, out_ref,
         got, own, stage, from_core, from_y, from_z,
         own_sem, g_recv, g_core, g_y, g_z, s_core, r_core, s_y, r_y, s_z, r_z) = refs
    tokens, dim = own.shape[1], own.shape[2]
    half = w1_ref.shape[0]
    me = lax.axis_index('expert')
    z, y, c = lax.div(me, 4), lax.rem(lax.div(me, 2), 2), lax.rem(me, 2)

    def at(zz, yy, cc):
        return (zz * 2 + yy) * 2 + cc

    other_core = at(z, y, 1 - c)
    other_y = at(z, 1 - y, c)

    upper, odd = lax.div(z, 2), lax.rem(z, 2)
    at_end = jnp.logical_or(z == 0, z == 3)
    inside = jnp.logical_and(z > 0, z < 3)

    def column(n):
        far = lax.div(n, 2)
        return far * (n + upper * (3 - 2 * n)) + (1 - far) * (2 * upper + lax.rem(odd + n, 2))

    right, left = at(lax.rem(z + 1, 4), y, c), at(lax.rem(z + 3, 4), y, c)

    def remote(src, dst, send, recv, peer):
        return pltpu.make_async_remote_copy(src_ref=src, dst_ref=dst, send_sem=send, recv_sem=recv, device_id={'expert': peer}, device_id_type=pl.DeviceIdType.MESH)

    barrier = pltpu.get_barrier_semaphore()
    for peer in (other_core, other_y, right, left):
        pl.semaphore_signal(barrier, inc=1, device_id={'expert': peer}, device_id_type=pl.DeviceIdType.MESH)
    load_own = pltpu.make_async_copy(rows_ref, got.at[me], own_sem)
    load_own.start()
    pl.semaphore_wait(barrier, 4)
    load_own.wait()

    def gather_to_core(slot, block):
        return remote(got.at[block], got.at[block], g_core.at[slot], g_recv.at[block], other_core)

    def gather_to_y(n, block):
        return remote(got.at[block], got.at[block], g_y.at[n], g_recv.at[block], other_y)

    def gather_along(sem, block, peer):
        return remote(got.at[block], got.at[block], g_z.at[sem], g_recv.at[block], peer)

    def arrived(block):
        remote(got.at[block], got.at[block], g_core.at[0], g_recv.at[block], other_core).wait_recv()

    def along_z(n, action):
        source = column(n)
        block = at(source, y, c)

        @pl.when(jnp.logical_and(source <= z, z < 3))
        def _():
            action(gather_along(n, block, right))

        @pl.when(jnp.logical_and(source >= z, z > 0))
        def _():
            action(gather_along(n if n else 4, block, left))

    def start(copy):
        copy.start()

    def sent(copy):
        copy.wait_send()

    along_z(0, start)
    gather_to_y(0, me).start()
    gather_to_core(0, me).start()

    def pass_on(n):
        block = at(column(n), y, c)
        arrived(block)
        along_z(n, start)
        gather_to_y(n, block).start()
        gather_to_core(n, block).start()

    def order(step):
        late = lax.div(step, 4)
        return step + late * (7 - 2 * step), late

    def pair_base(step):
        n, across = order(step)
        return at(column(n), lax.rem(y + across, 2), 0)

    if backward:
        slots = saved.shape[2] // 2

        def load_saved(step):
            start = pl.multiple_of(pair_base(step) * slots, 2 * slots)
            which = lax.rem(step, 2)
            return pltpu.make_async_copy(u_ref.at[:, pl.ds(start, 2 * slots), :], saved.at[which], load_sem.at[which])

        load_saved(0).start()
        acc1[...] = jnp.zeros_like(acc1)
        acc2[...] = jnp.zeros_like(acc2)
        acc3[...] = jnp.zeros_like(acc3)
    else:
        slots = tokens // 2

    sel = (lax.broadcasted_iota(jnp.int32, (16, 16), 1) == me).astype(BF16)
    slot_row = lax.broadcasted_iota(jnp.int32, (slots, tokens), 0).astype(F32)

    def masks(block):
        table = mm(sel, got[block, tokens:, :])
        plain, gated = [], []
        for e in range(half):
            hit = table[0:1, e * tokens:(e + 1) * tokens] == slot_row
            gate = table[0:1, (half + e) * tokens:(half + e + 1) * tokens]
            plain.append(jnp.where(hit, 1.0, 0.0).astype(BF16))
            gated.append(jnp.where(hit, gate, 0.0).astype(BF16))
        return jnp.concatenate(plain, axis=0), jnp.concatenate(gated, axis=0)

    def experts_forward(mine, theirs):
        marks = [masks(block) for block in (mine, theirs)]
        placed = [mm(marks[s][0], got[block, :tokens, :]).astype(BF16) for s, block in enumerate((mine, theirs))]
        outs = []
        for e in range(half):
            rows = jnp.concatenate([part[e * slots:(e + 1) * slots] for part in placed], axis=0)
            act_1 = mm(rows, w1_ref[e]).astype(BF16).astype(F32)
            act_3 = mm(rows, w3_ref[e]).astype(BF16).astype(F32)
            hidden = (act_1 * jax.nn.sigmoid(act_1) * act_3).astype(BF16)
            outs.append(mm(hidden, w2_ref[e]).astype(BF16))

        def combine(s):
            return mm_tn(marks[s][1], jnp.concatenate([out[s * slots:(s + 1) * slots] for out in outs], axis=0))

        return combine

    def experts_backward(mine, theirs, which):
        marks = [masks(block) for block in (mine, theirs)]
        placed = [mm(marks[s][1], got[block, :tokens, :]).astype(BF16) for s, block in enumerate((mine, theirs))]
        outs = []
        for e in range(half):
            rows = saved[which, e]
            d_out = jnp.concatenate([part[e * slots:(e + 1) * slots] for part in placed], axis=0)
            pre_1 = mm(rows, w1_ref[e]).astype(BF16).astype(F32)
            pre_3 = mm(rows, w3_ref[e]).astype(BF16).astype(F32)
            sigma = jax.nn.sigmoid(pre_1)
            silu_1 = pre_1 * sigma
            hidden = (silu_1 * pre_3).astype(BF16)
            acc2[e] += mm_tn(hidden, d_out)
            grad_hid = mm_nt(d_out, w2_ref[e]).astype(BF16).astype(F32)
            grad_a1 = (grad_hid * pre_3 * sigma * (1.0 + pre_1 * (1.0 - sigma))).astype(BF16)
            grad_a3 = (grad_hid * silu_1).astype(BF16)
            acc1[e] += mm_tn(rows, grad_a1)
            acc3[e] += mm_tn(rows, grad_a3)
            outs.append((mm_nt(grad_a1, w1_ref[e]) + mm_nt(grad_a3, w3_ref[e])).astype(BF16))

        def combine(s):
            return mm_tn(marks[s][0], jnp.concatenate([out[s * slots:(s + 1) * slots] for out in outs], axis=0))

        return combine

    def send_core(step):
        which = lax.rem(step, 2)
        return remote(stage.at[which], from_core.at[which], s_core.at[which], r_core.at[which], other_core)

    def send_y(n):
        return remote(own.at[4 + n], from_y.at[n], s_y.at[n], r_y.at[n], other_y)

    def take_y(n):
        send_y(n).wait_recv()
        own[n] += from_y[n]

    def chain(n, action):
        goal = column(n)

        @pl.when(goal > z)
        def _():
            action(remote(own.at[n], from_z.at[goal], s_z.at[n - 1], r_z.at[goal], right))

        @pl.when(goal == z - 1)
        def _():
            action(remote(own.at[n], from_z.at[4], s_z.at[n - 1], r_z.at[4], left))

        @pl.when(goal < z - 1)
        def _():
            action(remote(own.at[n], from_z.at[goal], s_z.at[n - 1], r_z.at[goal], left))

    def take_z(n, slot):
        remote(own.at[n], from_z.at[slot], s_z.at[0], r_z.at[slot], left).wait_recv()
        own[n] += from_z[slot]

    def step_body(step, carry):
        n, across = order(step)
        base = pair_base(step)
        which = lax.rem(step, 2)

        @pl.when(step == 1)
        def _():
            pass_on(1)

        @pl.when(jnp.logical_or(jnp.logical_and(step == 1, inside), jnp.logical_and(step == 2, at_end)))
        def _():
            pass_on(2)

        @pl.when(jnp.logical_or(jnp.logical_and(step == 2, inside), jnp.logical_and(step == 3, at_end)))
        def _():
            pass_on(3)

        @pl.when(jnp.logical_and(step >= 1, step <= 4))
        def _():
            block = at(column(step - 1), 1 - y, c)
            arrived(block)
            gather_to_core(3 + step, block).start()

        arrived(base + 1 - c)
        if backward:
            @pl.when(step < 7)
            def _():
                load_saved(step + 1).start()
            load_saved(step).wait()
            low, high = base, base + 1
            combine = experts_backward(low, high, which)
        else:
            low, high = base, base + 1
            combine = experts_forward(low, high)

        @pl.when(step >= 2)
        def _():
            send_core(step).wait_send()

        first, second = combine(0), combine(1)

        @pl.when(c == 0)
        def _():
            stage[which] = second
            own[across * 4 + n] = first

        @pl.when(c == 1)
        def _():
            stage[which] = first
            own[across * 4 + n] = second

        send_core(step).start()

        send_core(step).wait_recv()
        own[across * 4 + n] += from_core[which]

        @pl.when(across == 1)
        def _():
            send_y(n).start()

        @pl.when(step == 6)
        def _():
            take_y(3)

            @pl.when(at_end)
            def _():
                chain(3, start)

        return carry

    lax.fori_loop(0, 8, step_body, 0)
    if backward:
        stores = [pltpu.make_async_copy(acc, ref, store_sem.at[i]) for i, (acc, ref) in enumerate(((acc1, gw1_ref), (acc2, gw2_ref), (acc3, gw3_ref)))]
        for store in stores:
            store.start()

    def join(n):
        @pl.when(inside)
        def _():
            take_z(n, column(n))
            chain(n, start)

    join(3)
    for n in (2, 1):
        take_y(n)

        @pl.when(at_end)
        def _():
            chain(n, start)

        join(n)
    take_y(0)

    @pl.when(z > 0)
    def _():
        take_z(0, z)

    @pl.when(z < 3)
    def _():
        take_z(0, 4)

    out_ref[...] = own[0].astype(out_ref.dtype)
    for n in (3, 2, 1):
        chain(n, sent)
    for n in range(4):
        along_z(n, sent)
        send_y(n).wait_send()
        gather_to_y(n, me).wait_send()
    for slot in range(8):
        gather_to_core(slot, me).wait_send()
    send_core(0).wait_send()
    send_core(1).wait_send()
    if backward:
        for store in stores:
            store.wait()


def exchange(backward, rows, weights, tokens, saved=None):
    w_1, w_3, w_2 = weights
    dim = rows.shape[1]
    half, ff = w_1.shape[0], w_1.shape[2]
    dma = pltpu.SemaphoreType.DMA
    block = (tokens, dim)
    scratch = [
        pltpu.VMEM((16,) + rows.shape, BF16),
        pltpu.VMEM((8,) + block, F32),
        pltpu.VMEM((2,) + block, F32),
        pltpu.VMEM((2,) + block, F32),
        pltpu.VMEM((4,) + block, F32),
        pltpu.VMEM((5,) + block, F32),
    ]
    tail = [dma((16,)), dma((8,)), dma((4,)), dma((5,)), dma((2,)), dma((2,)), dma((4,)), dma((4,)), dma((3,)), dma((5,))]
    any_spec = pl.BlockSpec(memory_space=pl.ANY)
    vmem_spec = pl.BlockSpec(memory_space=pltpu.VMEM)
    if backward:
        slots = saved.shape[1] // 16
        scratch += [
            pltpu.VMEM((2, half, 2 * slots, dim), BF16),
            pltpu.VMEM((half, dim, ff), F32),
            pltpu.VMEM((half, ff, dim), F32),
            pltpu.VMEM((half, dim, ff), F32),
            dma(()), dma((2,)), dma((3,)),
        ]
        operands = (rows, saved, w_1, w_3, w_2)
        in_specs = [any_spec, any_spec, vmem_spec, vmem_spec, vmem_spec]
        out_shape = [jax.ShapeDtypeStruct(block, BF16), jax.ShapeDtypeStruct((half, dim, ff), F32), jax.ShapeDtypeStruct((half, ff, dim), F32), jax.ShapeDtypeStruct((half, dim, ff), F32)]
        out_specs = [vmem_spec, any_spec, any_spec, any_spec]
    else:
        scratch += [dma(())]
        operands = (rows, w_1, w_3, w_2)
        in_specs = [any_spec, vmem_spec, vmem_spec, vmem_spec]
        out_shape = [jax.ShapeDtypeStruct(block, F32)]
        out_specs = [vmem_spec]
    return pl.pallas_call(
        functools.partial(exchange_kernel, backward),
        out_shape=out_shape,
        in_specs=in_specs,
        out_specs=out_specs,
        scratch_shapes=scratch + tail,
        name='exchange_b' if backward else 'exchange_a',
        compiler_params=pltpu.CompilerParams(collective_id=1 if backward else 0, has_side_effects=True, vmem_limit_bytes=VMEM_BYTES),
    )(*operands)


def device_backward(x_dev, dy_dev, du_dev, norm_1, norm_2, w_q, w_k, w_v, w_o):
    attn_val, attn_pull = jax.vjp(attn_out, x_dev, norm_1, w_q, w_k, w_v, w_o)
    h_dev = add_rows(x_dev, attn_val)
    _, norm_pull = jax.vjp(rms_norm, h_dev, norm_2)
    dh_norm, grad_n2 = norm_pull(du_dev)
    dh_dev = add_rows(dy_dev, dh_norm)
    grad_x, grad_n1, grad_q, grad_k, grad_v, grad_o = attn_pull(dh_dev)
    return (add_rows(dh_dev, grad_x), grad_q.astype(jnp.float32), grad_k.astype(jnp.float32), grad_v.astype(jnp.float32), grad_o.astype(jnp.float32), grad_n1.astype(jnp.float32), grad_n2.astype(jnp.float32))


def solution(mesh):
    group = mesh.shape['expert']

    def local_step(x_a, x_b, dy_b, eid_a, slot_a, gate_a, eid_b, slot_b, gate_b, u_b, norm_1, norm_2, w_q, w_k, w_v, w_o, w_1, w_2, w_3):
        local_experts = w_1.shape[0]
        experts = local_experts * group
        model_dim = x_a.shape[1]

        tokens = x_a.shape[0]

        def with_routing(rows, expert_ids, slot_ids, gates):
            slots, weights = routing_table(expert_ids, slot_ids, gates, experts)
            table = jnp.stack([slots, weights], axis=1).reshape(tokens, 2, group, local_experts)
            table = table.transpose(2, 1, 3, 0).reshape(group, 2 * local_experts * tokens)
            table = jnp.pad(table, ((0, 0), (0, model_dim - table.shape[1])))
            return jnp.concatenate([rows, table], axis=0)

        weights = (w_1, w_3, w_2)
        du_rows, grad_w1, grad_w2, grad_w3 = exchange(True, with_routing(dy_b, eid_b, slot_b, gate_b), weights, tokens, u_b)
        h_a = add_rows(x_a, attn_out(x_a, norm_1, w_q, w_k, w_v, w_o))
        u_a = rms_norm(h_a, norm_2)
        mixed = exchange(False, with_routing(u_a, eid_a, slot_a, gate_a), weights, tokens)[0]
        y_a = (h_a.astype(jnp.float32) + mixed).astype(jnp.bfloat16)
        dx_b, g_q, g_k, g_v, g_o, g_n1, g_n2 = device_backward(x_b, dy_b, du_rows, norm_1, norm_2, w_q, w_k, w_v, w_o)
        return (y_a, dx_b, grad_w1, grad_w2, grad_w3, g_q[None], g_k[None], g_v[None], g_o[None], g_n1[None], g_n2[None])

    row_spec = P(('data', 'expert'), None)
    cube_spec = P(('data', 'expert'), None, None)
    quad_spec = P(('data', 'expert'), None, None, None)
    expert_spec = P('expert', None, None)
    in_specs = (row_spec, row_spec, row_spec, row_spec, row_spec, row_spec, row_spec, row_spec, row_spec, cube_spec, P(), P(), P(), P(), P(), P(), expert_spec, expert_spec, expert_spec)
    out_specs = (row_spec, row_spec, cube_spec, cube_spec, cube_spec, quad_spec, quad_spec, quad_spec, quad_spec, row_spec, row_spec)
    return jax.shard_map(local_step, mesh=mesh, in_specs=in_specs, out_specs=out_specs, check_vma=False)
```

```python
import functools

import jax
import jax.numpy as jnp
from jax import lax
from jax.experimental import pallas as pl
from jax.experimental.pallas import tpu as pltpu
from jax.sharding import PartitionSpec as P

F32 = jnp.float32
BF16 = jnp.bfloat16
VMEM_BYTES = 66_000_000

NORM_EPS = 1e-6


def routing_table(expert_ids, slot_ids, gates, experts):
    hit = (expert_ids[:, :, None] == jnp.arange(experts)[None, None, :]) & (slot_ids >= 0)[:, :, None]
    slots = jnp.sum(jnp.where(hit, slot_ids[:, :, None] + 1, 0), axis=1) - 1
    weights = jnp.sum(jnp.where(hit, gates.astype(jnp.float32)[:, :, None], 0.0), axis=1)
    return slots.astype(jnp.bfloat16), weights.astype(jnp.bfloat16)


def mm(left, right):
    return lax.dot_general(left, right, (((1,), (0,)), ((), ())), preferred_element_type=F32)


def mm_nt(left, right):
    return lax.dot_general(left, right, (((1,), (1,)), ((), ())), preferred_element_type=F32)


def mm_tn(left, right):
    return lax.dot_general(left, right, (((0,), (0,)), ((), ())), preferred_element_type=F32)


class Attention:
    def __init__(self, got, proj, ctx, x_ref, n1_ref, n2_ref, head_dim):
        self.got, self.proj, self.ctx, self.x_ref, self.n1_ref, self.n2_ref = got, proj, ctx, x_ref, n1_ref, n2_ref
        self.tokens, self.dim = x_ref.shape
        self.head_dim = head_dim
        self.kv = self.dim // 2
        self.chunk = self.dim // 4
        self.low = lax.broadcasted_iota(jnp.int32, (self.tokens, 2 * head_dim), 1) < head_dim
        row = lax.broadcasted_iota(jnp.int32, (2 * self.tokens, self.tokens), 0)
        row = jnp.where(row >= self.tokens, row - self.tokens, row)
        self.causal = row >= lax.broadcasted_iota(jnp.int32, (2 * self.tokens, self.tokens), 1)

    def copies(self, wq, wk, wv, wo, sems):
        n, out = self.chunk, []
        for i in range(4):
            rows = pl.ds(i * n, n)
            out.append(pltpu.make_async_copy(wq.at[rows], self.got.at[i, pl.ds(0, n)], sems.at[i]))
            out.append(pltpu.make_async_copy(wo.at[rows], self.got.at[4 + i, pl.ds(0, n)], sems.at[4 + i]))
            out.append(pltpu.make_async_copy(wk.at[rows], self.got.at[8 + i, pl.ds(0, n), pl.ds(0, self.kv)], sems.at[8 + i]))
            out.append(pltpu.make_async_copy(wv.at[rows], self.got.at[8 + i, pl.ds(0, n), pl.ds(self.kv, self.kv)], sems.at[12 + i]))
        return out

    def weight(self, i):
        return self.got[i, :self.chunk, :]

    def scale(self, wide):
        return lax.rsqrt(jnp.mean(wide * wide, axis=-1, keepdims=True) + NORM_EPS)

    def norm(self, wide, gain_ref):
        return (wide * self.scale(wide) * gain_ref[...].astype(F32)).astype(BF16)

    def norm_pull(self, wide, gain_ref, grad):
        inv = self.scale(wide)
        gain_grad = jnp.sum(grad * (wide * inv), axis=0, keepdims=True).astype(BF16).astype(F32)
        inner = grad * gain_ref[...].astype(F32)
        row_grad = inv * inner - wide * (inv * inv * inv * jnp.mean(inner * wide, axis=-1, keepdims=True))
        return row_grad.astype(BF16), gain_grad

    def normed(self):
        return self.norm(self.x_ref[...].astype(F32), self.n1_ref)

    def part(self, rows, i):
        return rows[:, i * self.chunk:(i + 1) * self.chunk]

    def project(self):
        rows = self.normed()
        self.proj[:, :self.dim] = sum(mm(self.part(rows, i), self.weight(i)) for i in range(4)).astype(BF16)
        self.proj[:, self.dim:] = sum(mm(self.part(rows, i), self.weight(8 + i)) for i in range(4)).astype(BF16)

    def stacked(self, ref, start):
        pair = ref[:, pl.ds(start, 2 * self.head_dim)].astype(F32)
        return jnp.concatenate([jnp.where(self.low, pair, 0.0), jnp.where(self.low, 0.0, pair)], axis=0).astype(BF16)

    def doubled(self, start, odd):
        pair = self.proj[:, pl.ds(start, 2 * self.head_dim)].astype(F32)
        turned = pltpu.roll(pair, self.head_dim, 1)
        return (jnp.where(self.low, turned, pair) if odd else jnp.where(self.low, pair, turned)).astype(BF16)

    def merged(self, both):
        return jnp.where(self.low, both[:self.tokens], both[self.tokens:])

    def group(self, quad, odd):
        width = 2 * self.head_dim
        at = pl.multiple_of((2 * quad + odd) * width, width)
        kv_at = pl.multiple_of(quad * width, width)
        query = self.stacked(self.proj, at)
        keys = self.doubled(self.dim + kv_at, odd)
        vals = self.doubled(self.dim + self.kv + kv_at, odd)
        scores = jnp.where(self.causal, mm_nt(query, keys) * self.head_dim ** -0.5, -1e30)
        powers = jnp.exp(scores - jnp.max(scores, axis=-1, keepdims=True))
        return at, kv_at, query, keys, vals, powers / jnp.sum(powers, axis=-1, keepdims=True)

    def heads(self):
        def body(quad, carry):
            for odd in range(2):
                at, _, _, _, vals, probs = self.group(quad, odd)
                self.ctx[:, pl.ds(at, 2 * self.head_dim)] = self.merged(mm(probs.astype(BF16), vals)).astype(BF16)
            return carry

        lax.fori_loop(0, self.kv // (2 * self.head_dim), body, 0)

    def hidden(self):
        attn = sum(mm(self.part(self.ctx[...], i), self.weight(4 + i)) for i in range(4)).astype(BF16)
        return (self.x_ref[...].astype(F32) + attn.astype(F32)).astype(BF16)

    def pull_heads(self, d_ctx, d_proj):
        def fold(both):
            return both + pltpu.roll(both, self.head_dim, 1)

        def body(quad, carry):
            d_keys, d_vals = [], []
            for odd in range(2):
                at, kv_at, query, keys, vals, probs = self.group(quad, odd)
                grad = self.stacked(d_ctx, at)
                d_probs = mm_nt(grad, vals).astype(BF16).astype(F32)
                d_vals.append(fold(mm_tn(probs.astype(BF16), grad)))
                d_scores = probs * (d_probs - jnp.sum(probs * d_probs, axis=-1, keepdims=True))
                d_scores = (jnp.where(self.causal, d_scores, 0.0) * self.head_dim ** -0.5).astype(BF16)
                d_proj[:, pl.ds(at, 2 * self.head_dim)] = self.merged(mm(d_scores, keys)).astype(BF16)
                d_keys.append(fold(mm_tn(d_scores, query)))
            d_proj[:, pl.ds(self.dim + kv_at, 2 * self.head_dim)] = jnp.where(self.low, d_keys[0], d_keys[1]).astype(BF16)
            d_proj[:, pl.ds(self.dim + self.kv + kv_at, 2 * self.head_dim)] = jnp.where(self.low, d_vals[0], d_vals[1]).astype(BF16)
            return carry

        lax.fori_loop(0, self.kv // (2 * self.head_dim), body, 0)


def exchange_kernel(backward, head_dim, *refs):
    if backward:
        (rows_ref, u_ref, w1_ref, w3_ref, w2_ref, x_ref, n1_ref, n2_ref, wq_ref, wk_ref, wv_ref, wo_ref,
         out_ref, gw1_ref, gw2_ref, gw3_ref, h_ref, norm_ref, proj, ctx, att_sem, got, own, stage, from_core, from_y, from_z, saved, acc1, acc2, acc3,
         own_sem, load_sem, store_sem, g_recv, g_core, g_y, g_z, s_core, r_core, s_y, r_y, s_z, r_z) = refs
    else:
        (rows_ref, w1_ref, w3_ref, w2_ref, x_ref, n1_ref, n2_ref, wq_ref, wk_ref, wv_ref, wo_ref, dy_ref, du_ref,
         out_ref, dx_ref, gq_ref, gk_ref, gv_ref, go_ref, gn1_ref, gn2_ref, proj, ctx, att_sem, d_ctx, d_proj, got, own, stage, from_core, from_y, from_z,
         own_sem, g_recv, g_core, g_y, g_z, s_core, r_core, s_y, r_y, s_z, r_z) = refs
    tokens, dim = own.shape[1], own.shape[2]
    half = w1_ref.shape[0]
    me = lax.axis_index('expert')
    z, y, c = lax.div(me, 4), lax.rem(lax.div(me, 2), 2), lax.rem(me, 2)

    def at(zz, yy, cc):
        return (zz * 2 + yy) * 2 + cc

    other_core = at(z, y, 1 - c)
    other_y = at(z, 1 - y, c)

    upper, odd = lax.div(z, 2), lax.rem(z, 2)
    at_end = jnp.logical_or(z == 0, z == 3)
    inside = jnp.logical_and(z > 0, z < 3)

    def column(n):
        far = lax.div(n, 2)
        return far * (n + upper * (3 - 2 * n)) + (1 - far) * (2 * upper + lax.rem(odd + n, 2))

    right, left = at(lax.rem(z + 1, 4), y, c), at(lax.rem(z + 3, 4), y, c)

    def remote(src, dst, send, recv, peer):
        return pltpu.make_async_remote_copy(src_ref=src, dst_ref=dst, send_sem=send, recv_sem=recv, device_id={'expert': peer}, device_id_type=pl.DeviceIdType.MESH)

    barrier = pltpu.get_barrier_semaphore()
    for peer in (other_core, other_y, right, left):
        pl.semaphore_signal(barrier, inc=1, device_id={'expert': peer}, device_id_type=pl.DeviceIdType.MESH)
    load_own = pltpu.make_async_copy(rows_ref, got.at[me], own_sem)
    load_own.start()
    pl.semaphore_wait(barrier, 4)
    load_own.wait()

    def gather_to_core(slot, block):
        return remote(got.at[block], got.at[block], g_core.at[slot], g_recv.at[block], other_core)

    def gather_to_y(n, block):
        return remote(got.at[block], got.at[block], g_y.at[n], g_recv.at[block], other_y)

    def gather_along(sem, block, peer):
        return remote(got.at[block], got.at[block], g_z.at[sem], g_recv.at[block], peer)

    def arrived(block):
        remote(got.at[block], got.at[block], g_core.at[0], g_recv.at[block], other_core).wait_recv()

    def along_z(n, action):
        source = column(n)
        block = at(source, y, c)

        @pl.when(jnp.logical_and(source <= z, z < 3))
        def _():
            action(gather_along(n, block, right))

        @pl.when(jnp.logical_and(source >= z, z > 0))
        def _():
            action(gather_along(n if n else 4, block, left))

    def start(copy):
        copy.start()

    def sent(copy):
        copy.wait_send()

    along_z(0, start)
    gather_to_y(0, me).start()
    gather_to_core(0, me).start()

    def pass_on(n):
        block = at(column(n), y, c)
        arrived(block)
        along_z(n, start)
        gather_to_y(n, block).start()
        gather_to_core(n, block).start()

    def order(step):
        late = lax.div(step, 4)
        return step + late * (7 - 2 * step), late

    def pair_base(step):
        n, across = order(step)
        return at(column(n), lax.rem(y + across, 2), 0)

    if backward:
        slots = saved.shape[2] // 2

        def load_saved(step):
            start = pl.multiple_of(pair_base(step) * slots, 2 * slots)
            which = lax.rem(step, 2)
            return pltpu.make_async_copy(u_ref.at[:, pl.ds(start, 2 * slots), :], saved.at[which], load_sem.at[which])

        load_saved(0).start()
        acc1[...] = jnp.zeros_like(acc1)
        acc2[...] = jnp.zeros_like(acc2)
        acc3[...] = jnp.zeros_like(acc3)
    else:
        slots = tokens // 2

    sel = (lax.broadcasted_iota(jnp.int32, (16, 16), 1) == me).astype(BF16)
    slot_row = lax.broadcasted_iota(jnp.int32, (slots, tokens), 0).astype(F32)

    def masks(block):
        table = mm(sel, got[block, tokens:, :])
        plain, gated = [], []
        for e in range(half):
            hit = table[0:1, e * tokens:(e + 1) * tokens] == slot_row
            gate = table[0:1, (half + e) * tokens:(half + e + 1) * tokens]
            plain.append(jnp.where(hit, 1.0, 0.0).astype(BF16))
            gated.append(jnp.where(hit, gate, 0.0).astype(BF16))
        return jnp.concatenate(plain, axis=0), jnp.concatenate(gated, axis=0)

    def experts_forward(mine, theirs):
        marks = [masks(block) for block in (mine, theirs)]
        placed = [mm(marks[s][0], got[block, :tokens, :]).astype(BF16) for s, block in enumerate((mine, theirs))]
        outs = []
        for e in range(half):
            rows = jnp.concatenate([part[e * slots:(e + 1) * slots] for part in placed], axis=0)
            act_1 = mm(rows, w1_ref[e]).astype(BF16).astype(F32)
            act_3 = mm(rows, w3_ref[e]).astype(BF16).astype(F32)
            hidden = (act_1 * jax.nn.sigmoid(act_1) * act_3).astype(BF16)
            outs.append(mm(hidden, w2_ref[e]).astype(BF16))

        def combine(s):
            return mm_tn(marks[s][1], jnp.concatenate([out[s * slots:(s + 1) * slots] for out in outs], axis=0))

        return combine

    def experts_backward(mine, theirs, which):
        marks = [masks(block) for block in (mine, theirs)]
        placed = [mm(marks[s][1], got[block, :tokens, :]).astype(BF16) for s, block in enumerate((mine, theirs))]
        outs = []
        for e in range(half):
            rows = saved[which, e]
            d_out = jnp.concatenate([part[e * slots:(e + 1) * slots] for part in placed], axis=0)
            pre_1 = mm(rows, w1_ref[e]).astype(BF16).astype(F32)
            pre_3 = mm(rows, w3_ref[e]).astype(BF16).astype(F32)
            sigma = jax.nn.sigmoid(pre_1)
            silu_1 = pre_1 * sigma
            hidden = (silu_1 * pre_3).astype(BF16)
            acc2[e] += mm_tn(hidden, d_out)
            grad_hid = mm_nt(d_out, w2_ref[e]).astype(BF16).astype(F32)
            grad_a1 = (grad_hid * pre_3 * sigma * (1.0 + pre_1 * (1.0 - sigma))).astype(BF16)
            grad_a3 = (grad_hid * silu_1).astype(BF16)
            acc1[e] += mm_tn(rows, grad_a1)
            acc3[e] += mm_tn(rows, grad_a3)
            outs.append((mm_nt(grad_a1, w1_ref[e]) + mm_nt(grad_a3, w3_ref[e])).astype(BF16))

        def combine(s):
            return mm_tn(marks[s][0], jnp.concatenate([out[s * slots:(s + 1) * slots] for out in outs], axis=0))

        return combine

    def send_core(step):
        which = lax.rem(step, 2)
        return remote(stage.at[which], from_core.at[which], s_core.at[which], r_core.at[which], other_core)

    def send_y(n):
        return remote(own.at[4 + n], from_y.at[n], s_y.at[n], r_y.at[n], other_y)

    def take_y(n):
        send_y(n).wait_recv()
        own[n] += from_y[n]

    def chain(n, action):
        goal = column(n)

        @pl.when(goal > z)
        def _():
            action(remote(own.at[n], from_z.at[goal], s_z.at[n - 1], r_z.at[goal], right))

        @pl.when(goal == z - 1)
        def _():
            action(remote(own.at[n], from_z.at[4], s_z.at[n - 1], r_z.at[4], left))

        @pl.when(goal < z - 1)
        def _():
            action(remote(own.at[n], from_z.at[goal], s_z.at[n - 1], r_z.at[goal], left))

    def take_z(n, slot):
        remote(own.at[n], from_z.at[slot], s_z.at[0], r_z.at[slot], left).wait_recv()
        own[n] += from_z[slot]

    def step_body(step, carry):
        n, across = order(step)
        base = pair_base(step)
        which = lax.rem(step, 2)

        @pl.when(step == 1)
        def _():
            pass_on(1)

        @pl.when(jnp.logical_or(jnp.logical_and(step == 1, inside), jnp.logical_and(step == 2, at_end)))
        def _():
            pass_on(2)

        @pl.when(jnp.logical_or(jnp.logical_and(step == 2, inside), jnp.logical_and(step == 3, at_end)))
        def _():
            pass_on(3)

        @pl.when(jnp.logical_and(step >= 1, step <= 4))
        def _():
            block = at(column(step - 1), 1 - y, c)
            arrived(block)
            gather_to_core(3 + step, block).start()

        arrived(base + 1 - c)
        if backward:
            @pl.when(step < 7)
            def _():
                load_saved(step + 1).start()
            load_saved(step).wait()
            low, high = base, base + 1
            combine = experts_backward(low, high, which)
        else:
            low, high = base, base + 1
            combine = experts_forward(low, high)

        @pl.when(step >= 2)
        def _():
            send_core(step).wait_send()

        first, second = combine(0), combine(1)

        @pl.when(c == 0)
        def _():
            stage[which] = second
            own[across * 4 + n] = first

        @pl.when(c == 1)
        def _():
            stage[which] = first
            own[across * 4 + n] = second

        send_core(step).start()

        send_core(step).wait_recv()
        own[across * 4 + n] += from_core[which]

        @pl.when(across == 1)
        def _():
            send_y(n).start()

        @pl.when(step == 6)
        def _():
            take_y(3)

            @pl.when(at_end)
            def _():
                chain(3, start)

        return carry

    lax.fori_loop(0, 8, step_body, 0)
    if backward:
        stores = [pltpu.make_async_copy(acc, ref, store_sem.at[i]) for i, (acc, ref) in enumerate(((acc1, gw1_ref), (acc2, gw2_ref), (acc3, gw3_ref)))]
        for store in stores:
            store.start()

    for n in range(4):
        along_z(n, sent)
        gather_to_y(n, me).wait_send()
    for slot in range(8):
        gather_to_core(slot, me).wait_send()
    attention = Attention(got, proj, ctx, x_ref, n1_ref, n2_ref, head_dim)
    weights = attention.copies(wq_ref, wk_ref, wv_ref, wo_ref, att_sem)
    for copy in weights:
        copy.start()

    def join(n):
        @pl.when(inside)
        def _():
            take_z(n, column(n))
            chain(n, start)

    def pass_sum(n):
        take_y(n)

        @pl.when(at_end)
        def _():
            chain(n, start)

    if not backward:
        for copy in weights:
            copy.wait()
        attention.project()
        attention.heads()
        hid = attention.hidden()
        d_norm, gn2_ref[...] = attention.norm_pull(hid.astype(F32), n2_ref, du_ref[...].astype(F32))
        d_hid = (dy_ref[...].astype(F32) + d_norm.astype(F32)).astype(BF16)
        dx_ref[...] = d_hid
        for i in range(4):
            d_ctx[:, i * attention.chunk:(i + 1) * attention.chunk] = mm_nt(d_hid, attention.weight(4 + i)).astype(BF16)
        for i in range(4):
            go_ref[pl.ds(i * attention.chunk, attention.chunk), :] = mm_tn(attention.part(ctx[...], i), d_hid).astype(BF16)
    join(3)
    if backward:
        for copy in weights:
            copy.wait()
        attention.project()
    pass_sum(2)
    join(2)
    if backward:
        attention.heads()
    else:
        attention.pull_heads(d_ctx, d_proj)
    pass_sum(1)
    join(1)
    kv = attention.kv
    if backward:
        hid = attention.hidden()
        h_ref[...] = hid
        norm_ref[...] = attention.norm(hid.astype(F32), n2_ref)
    else:
        rows = attention.normed()
        for i in range(4):
            block = pl.ds(i * attention.chunk, attention.chunk)
            gq_ref[block, :] = mm_tn(attention.part(rows, i), d_proj[:, :dim]).astype(BF16)
            gk_ref[block, :] = mm_tn(attention.part(rows, i), d_proj[:, dim:dim + kv]).astype(BF16)
            gv_ref[block, :] = mm_tn(attention.part(rows, i), d_proj[:, dim + kv:]).astype(BF16)
        pulled = [mm_nt(d_proj[:, :dim], attention.weight(i)) + mm_nt(d_proj[:, dim:], attention.weight(8 + i)) for i in range(4)]
        d_rows = jnp.concatenate(pulled, axis=1).astype(BF16).astype(F32)
        d_x, gn1_ref[...] = attention.norm_pull(x_ref[...].astype(F32), n1_ref, d_rows)
        dx_ref[...] = (dx_ref[...].astype(F32) + d_x.astype(F32)).astype(BF16)
    take_y(0)

    @pl.when(z > 0)
    def _():
        take_z(0, z)

    @pl.when(z < 3)
    def _():
        take_z(0, 4)

    out_ref[...] = own[0].astype(out_ref.dtype)
    for n in (3, 2, 1):
        chain(n, sent)
    for n in range(4):
        send_y(n).wait_send()
    send_core(0).wait_send()
    send_core(1).wait_send()
    if backward:
        for store in stores:
            store.wait()


def exchange(backward, rows, weights, tokens, head_dim, sequence, saved=None):
    w_1, w_3, w_2 = weights
    dim = rows.shape[1]
    half, ff = w_1.shape[0], w_1.shape[2]
    dma = pltpu.SemaphoreType.DMA
    block = (tokens, dim)
    model = (dim, dim)
    narrow = (dim, dim // 2)
    scratch = [
        pltpu.VMEM((tokens, 2 * dim), BF16),
        pltpu.VMEM(block, BF16),
        dma((16,)),
    ]
    if not backward:
        scratch += [pltpu.VMEM(block, BF16), pltpu.VMEM((tokens, 2 * dim), BF16)]
    scratch += [
        pltpu.VMEM((16,) + rows.shape, BF16),
        pltpu.VMEM((8,) + block, F32),
        pltpu.VMEM((2,) + block, F32),
        pltpu.VMEM((2,) + block, F32),
        pltpu.VMEM((4,) + block, F32),
        pltpu.VMEM((5,) + block, F32),
    ]
    tail = [dma((16,)), dma((8,)), dma((4,)), dma((5,)), dma((2,)), dma((2,)), dma((4,)), dma((4,)), dma((3,)), dma((5,))]
    any_spec = pl.BlockSpec(memory_space=pl.ANY)
    vmem_spec = pl.BlockSpec(memory_space=pltpu.VMEM)
    if backward:
        slots = saved.shape[1] // 16
        scratch += [
            pltpu.VMEM((2, half, 2 * slots, dim), BF16),
            pltpu.VMEM((half, dim, ff), F32),
            pltpu.VMEM((half, ff, dim), F32),
            pltpu.VMEM((half, dim, ff), F32),
            dma(()), dma((2,)), dma((3,)),
        ]
        operands = (rows, saved, w_1, w_3, w_2) + sequence
        in_specs = [any_spec, any_spec] + [vmem_spec] * 6 + [any_spec] * 4
        out_shape = [jax.ShapeDtypeStruct(block, BF16), jax.ShapeDtypeStruct((half, dim, ff), F32), jax.ShapeDtypeStruct((half, ff, dim), F32), jax.ShapeDtypeStruct((half, dim, ff), F32), jax.ShapeDtypeStruct(block, BF16), jax.ShapeDtypeStruct(block, BF16)]
        out_specs = [vmem_spec, any_spec, any_spec, any_spec, vmem_spec, vmem_spec]
    else:
        scratch += [dma(())]
        operands = (rows, w_1, w_3, w_2) + sequence
        in_specs = [any_spec] + [vmem_spec] * 6 + [any_spec] * 4 + [vmem_spec] * 2
        out_shape = [jax.ShapeDtypeStruct(block, F32), jax.ShapeDtypeStruct(block, BF16)]
        out_shape += [jax.ShapeDtypeStruct(shape, BF16) for shape in (model, narrow, narrow, model)]
        out_shape += [jax.ShapeDtypeStruct((1, dim), F32)] * 2
        out_specs = [vmem_spec] * 8
    return pl.pallas_call(
        functools.partial(exchange_kernel, backward, head_dim),
        out_shape=out_shape,
        in_specs=in_specs,
        out_specs=out_specs,
        scratch_shapes=scratch + tail,
        name='exchange_b' if backward else 'exchange_a',
        compiler_params=pltpu.CompilerParams(collective_id=1 if backward else 0, has_side_effects=True, vmem_limit_bytes=VMEM_BYTES),
    )(*operands)


def solution(mesh):
    group = mesh.shape['expert']

    def local_step(x_a, x_b, dy_b, eid_a, slot_a, gate_a, eid_b, slot_b, gate_b, u_b, norm_1, norm_2, w_q, w_k, w_v, w_o, w_1, w_2, w_3):
        local_experts = w_1.shape[0]
        experts = local_experts * group
        model_dim = x_a.shape[1]

        tokens = x_a.shape[0]

        def with_routing(rows, expert_ids, slot_ids, gates):
            slots, weights = routing_table(expert_ids, slot_ids, gates, experts)
            table = jnp.stack([slots, weights], axis=1).reshape(tokens, 2, group, local_experts)
            table = table.transpose(2, 1, 3, 0).reshape(group, 2 * local_experts * tokens)
            table = jnp.pad(table, ((0, 0), (0, model_dim - table.shape[1])))
            return jnp.concatenate([rows, table], axis=0)

        weights = (w_1, w_3, w_2)
        head_dim = w_q.shape[2]
        layer = (norm_1[None], norm_2[None], w_q.reshape(model_dim, -1), w_k.reshape(model_dim, -1), w_v.reshape(model_dim, -1), w_o.reshape(-1, model_dim))
        du_rows, grad_w1, grad_w2, grad_w3, h_a, u_a = exchange(True, with_routing(dy_b, eid_b, slot_b, gate_b), weights, tokens, head_dim, (x_a,) + layer, u_b)
        mixed, dx_b, g_q, g_k, g_v, g_o, g_n1, g_n2 = exchange(False, with_routing(u_a, eid_a, slot_a, gate_a), weights, tokens, head_dim, (x_b,) + layer + (dy_b, du_rows))
        y_a = (h_a.astype(jnp.float32) + mixed).astype(jnp.bfloat16)
        g_q, g_k, g_v, g_o = (grad.astype(jnp.float32).reshape(weight.shape) for grad, weight in ((g_q, w_q), (g_k, w_k), (g_v, w_v), (g_o, w_o)))
        g_n1, g_n2 = g_n1[0], g_n2[0]
        return (y_a, dx_b, grad_w1, grad_w2, grad_w3, g_q[None], g_k[None], g_v[None], g_o[None], g_n1[None], g_n2[None])

    row_spec = P(('data', 'expert'), None)
    cube_spec = P(('data', 'expert'), None, None)
    quad_spec = P(('data', 'expert'), None, None, None)
    expert_spec = P('expert', None, None)
    in_specs = (row_spec, row_spec, row_spec, row_spec, row_spec, row_spec, row_spec, row_spec, row_spec, cube_spec, P(), P(), P(), P(), P(), P(), expert_spec, expert_spec, expert_spec)
    out_specs = (row_spec, row_spec, cube_spec, cube_spec, cube_spec, quad_spec, quad_spec, quad_spec, quad_spec, row_spec, row_spec)
    return jax.shard_map(local_step, mesh=mesh, in_specs=in_specs, out_specs=out_specs, check_vma=False)
```

```python
import functools

import jax
import jax.numpy as jnp
from jax import lax
from jax.experimental import pallas as pl
from jax.experimental.pallas import tpu as pltpu
from jax.sharding import PartitionSpec as P

F32 = jnp.float32
BF16 = jnp.bfloat16
VMEM_BYTES = 66_000_000
SIDE = 4

NORM_EPS = 1e-6


def mm(left, right):
    return lax.dot_general(left, right, (((1,), (0,)), ((), ())), preferred_element_type=F32)


def mm_nt(left, right):
    return lax.dot_general(left, right, (((1,), (1,)), ((), ())), preferred_element_type=F32)


def mm_tn(left, right):
    return lax.dot_general(left, right, (((0,), (0,)), ((), ())), preferred_element_type=F32)


class Attention:
    def __init__(self, got, proj, ctx, x_ref, gain_1, gain_2, head_dim):
        self.got, self.proj, self.ctx, self.x_ref, self.gain_1, self.gain_2 = got, proj, ctx, x_ref, gain_1, gain_2
        self.tokens, self.dim = x_ref.shape
        self.head_dim = head_dim
        self.kv = self.dim // 2
        self.chunk = self.dim // 4
        self.low = lax.broadcasted_iota(jnp.int32, (self.tokens, 2 * head_dim), 1) < head_dim
        row = lax.broadcasted_iota(jnp.int32, (2 * self.tokens, self.tokens), 0)
        row = jnp.where(row >= self.tokens, row - self.tokens, row)
        self.causal = row >= lax.broadcasted_iota(jnp.int32, (2 * self.tokens, self.tokens), 1)

    def copies(self, wq, wk, wv, wo, sems):
        n, out = self.chunk, []
        for i in range(4):
            rows = pl.ds(i * n, n)
            out.append(pltpu.make_async_copy(wq.at[rows], self.got.at[i, pl.ds(0, n)], sems.at[i]))
            out.append(pltpu.make_async_copy(wo.at[rows], self.got.at[4 + i, pl.ds(0, n)], sems.at[4 + i]))
            out.append(pltpu.make_async_copy(wk.at[rows], self.got.at[8 + i, pl.ds(0, n), pl.ds(0, self.kv)], sems.at[8 + i]))
            out.append(pltpu.make_async_copy(wv.at[rows], self.got.at[8 + i, pl.ds(0, n), pl.ds(self.kv, self.kv)], sems.at[12 + i]))
        return out

    def weight(self, i):
        return self.got[i, :self.chunk, :]

    def scale(self, wide):
        return lax.rsqrt(jnp.mean(wide * wide, axis=-1, keepdims=True) + NORM_EPS)

    def norm(self, wide, gain):
        return (wide * self.scale(wide) * gain).astype(BF16)

    def norm_pull(self, wide, gain, grad):
        inv = self.scale(wide)
        gain_grad = jnp.sum(grad * (wide * inv), axis=0, keepdims=True).astype(BF16).astype(F32)
        inner = grad * gain
        row_grad = inv * inner - wide * (inv * inv * inv * jnp.mean(inner * wide, axis=-1, keepdims=True))
        return row_grad.astype(BF16), gain_grad

    def normed(self):
        return self.norm(self.x_ref[...].astype(F32), self.gain_1)

    def part(self, rows, i):
        return rows[:, i * self.chunk:(i + 1) * self.chunk]

    def project(self):
        rows = self.normed()
        self.proj[:, :self.dim] = sum(mm(self.part(rows, i), self.weight(i)) for i in range(4)).astype(BF16)
        self.proj[:, self.dim:] = sum(mm(self.part(rows, i), self.weight(8 + i)) for i in range(4)).astype(BF16)

    def stacked(self, ref, start):
        pair = ref[:, pl.ds(start, 2 * self.head_dim)].astype(F32)
        return jnp.concatenate([jnp.where(self.low, pair, 0.0), jnp.where(self.low, 0.0, pair)], axis=0).astype(BF16)

    def doubled(self, start, odd):
        pair = self.proj[:, pl.ds(start, 2 * self.head_dim)].astype(F32)
        turned = pltpu.roll(pair, self.head_dim, 1)
        return (jnp.where(self.low, turned, pair) if odd else jnp.where(self.low, pair, turned)).astype(BF16)

    def merged(self, both):
        return jnp.where(self.low, both[:self.tokens], both[self.tokens:])

    def group(self, quad, odd):
        width = 2 * self.head_dim
        at = pl.multiple_of((2 * quad + odd) * width, width)
        kv_at = pl.multiple_of(quad * width, width)
        query = self.stacked(self.proj, at)
        keys = self.doubled(self.dim + kv_at, odd)
        vals = self.doubled(self.dim + self.kv + kv_at, odd)
        scores = jnp.where(self.causal, mm_nt(query, keys) * self.head_dim ** -0.5, -1e30)
        powers = jnp.exp(scores - jnp.max(scores, axis=-1, keepdims=True))
        return at, kv_at, query, keys, vals, powers / jnp.sum(powers, axis=-1, keepdims=True)

    def heads(self):
        def body(quad, carry):
            for odd in range(2):
                at, _, _, _, vals, probs = self.group(quad, odd)
                self.ctx[:, pl.ds(at, 2 * self.head_dim)] = self.merged(mm(probs.astype(BF16), vals)).astype(BF16)
            return carry

        lax.fori_loop(0, self.kv // (2 * self.head_dim), body, 0)

    def hidden(self):
        attn = sum(mm(self.part(self.ctx[...], i), self.weight(4 + i)) for i in range(4)).astype(BF16)
        return (self.x_ref[...].astype(F32) + attn.astype(F32)).astype(BF16)

    def pull_heads(self, d_ctx, d_proj):
        def fold(both):
            return both + pltpu.roll(both, self.head_dim, 1)

        def body(quad, carry):
            d_keys, d_vals = [], []
            for odd in range(2):
                at, kv_at, query, keys, vals, probs = self.group(quad, odd)
                grad = self.stacked(d_ctx, at)
                d_probs = mm_nt(grad, vals).astype(BF16).astype(F32)
                d_vals.append(fold(mm_tn(probs.astype(BF16), grad)))
                d_scores = probs * (d_probs - jnp.sum(probs * d_probs, axis=-1, keepdims=True))
                d_scores = (jnp.where(self.causal, d_scores, 0.0) * self.head_dim ** -0.5).astype(BF16)
                d_proj[:, pl.ds(at, 2 * self.head_dim)] = self.merged(mm(d_scores, keys)).astype(BF16)
                d_keys.append(fold(mm_tn(d_scores, query)))
            d_proj[:, pl.ds(self.dim + kv_at, 2 * self.head_dim)] = jnp.where(self.low, d_keys[0], d_keys[1]).astype(BF16)
            d_proj[:, pl.ds(self.dim + self.kv + kv_at, 2 * self.head_dim)] = jnp.where(self.low, d_vals[0], d_vals[1]).astype(BF16)
            return carry

        lax.fori_loop(0, self.kv // (2 * self.head_dim), body, 0)


def exchange_kernel(backward, head_dim, choices, *refs):
    if backward:
        (rows_ref, u_ref, w1_ref, w3_ref, w2_ref, x_ref, wq_ref, wk_ref, wv_ref, wo_ref,
         out_ref, gw1_ref, gw2_ref, gw3_ref, h_ref, norm_ref, proj, ctx, att_sem, got, own, stage, from_core, from_y, from_z, saved, acc1, acc2, acc3,
         own_sem, load_sem, store_sem, side_z, side_y, sz_send, sz_recv, sy_send, sy_recv, g_recv, g_core, g_y, g_z, s_core, r_core, s_y, r_y, s_z, r_z) = refs
    else:
        (rows_ref, w1_ref, w3_ref, w2_ref, x_ref, wq_ref, wk_ref, wv_ref, wo_ref, dy_ref, du_ref,
         out_ref, dx_ref, gq_ref, gk_ref, gv_ref, go_ref, gn1_ref, gn2_ref, proj, ctx, att_sem, d_ctx, d_proj, got, own, stage, from_core, from_y, from_z,
         own_sem, side_z, side_y, sz_send, sz_recv, sy_send, sy_recv, g_recv, g_core, g_y, g_z, s_core, r_core, s_y, r_y, s_z, r_z) = refs
    tokens, dim = own.shape[1], own.shape[2]
    half = w1_ref.shape[0]
    main = dim - dim // SIDE
    first, last = pl.ds(0, main), pl.ds(main, dim - main)
    me = lax.axis_index('expert')
    z, y, c = lax.div(me, 4), lax.rem(lax.div(me, 2), 2), lax.rem(me, 2)

    def at(zz, yy, cc):
        return (zz * 2 + yy) * 2 + cc

    other_core = at(z, y, 1 - c)
    other_y = at(z, 1 - y, c)

    upper, odd = lax.div(z, 2), lax.rem(z, 2)
    at_end = jnp.logical_or(z == 0, z == 3)
    inside = jnp.logical_and(z > 0, z < 3)

    def column(n):
        far = lax.div(n, 2)
        return far * (n + upper * (3 - 2 * n)) + (1 - far) * (2 * upper + lax.rem(odd + n, 2))

    right, left = at(lax.rem(z + 1, 4), y, c), at(lax.rem(z + 3, 4), y, c)

    def remote(src, dst, send, recv, peer):
        return pltpu.make_async_remote_copy(src_ref=src, dst_ref=dst, send_sem=send, recv_sem=recv, device_id={'expert': peer}, device_id_type=pl.DeviceIdType.MESH)

    barrier = pltpu.get_barrier_semaphore()
    for peer in (other_core, other_y, right, left):
        pl.semaphore_signal(barrier, inc=1, device_id={'expert': peer}, device_id_type=pl.DeviceIdType.MESH)
    load_own = pltpu.make_async_copy(rows_ref, got.at[me], own_sem)
    load_own.start()
    pl.semaphore_wait(barrier, 4)
    load_own.wait()

    def gather_to_core(slot, block):
        return remote(got.at[block], got.at[block], g_core.at[slot], g_recv.at[block], other_core)

    def gather_to_y(n, block):
        return remote(got.at[block], got.at[block], g_y.at[n], g_recv.at[block], other_y)

    def gather_along(sem, block, peer):
        return remote(got.at[block], got.at[block], g_z.at[sem], g_recv.at[block], peer)

    def arrived(block):
        remote(got.at[block], got.at[block], g_core.at[0], g_recv.at[block], other_core).wait_recv()

    def along_z(n, action):
        source = column(n)
        block = at(source, y, c)

        @pl.when(jnp.logical_and(source <= z, z < 3))
        def _():
            action(gather_along(n, block, right))

        @pl.when(jnp.logical_and(source >= z, z > 0))
        def _():
            action(gather_along(n if n else 4, block, left))

    def start(copy):
        copy.start()

    def sent(copy):
        copy.wait_send()

    along_z(0, start)
    gather_to_y(0, me).start()
    gather_to_core(0, me).start()

    def pass_on(n):
        block = at(column(n), y, c)
        arrived(block)
        along_z(n, start)
        gather_to_y(n, block).start()
        gather_to_core(n, block).start()

    def order(step):
        late = lax.div(step, 4)
        return step + late * (7 - 2 * step), late

    def pair_base(step):
        n, across = order(step)
        return at(column(n), lax.rem(y + across, 2), 0)

    if backward:
        slots = saved.shape[2] // 2

        def load_saved(step):
            start = pl.multiple_of(pair_base(step) * slots, 2 * slots)
            which = lax.rem(step, 2)
            return pltpu.make_async_copy(u_ref.at[:, pl.ds(start, 2 * slots), :], saved.at[which], load_sem.at[which])

        load_saved(0).start()
        acc1[...] = jnp.zeros_like(acc1)
        acc2[...] = jnp.zeros_like(acc2)
        acc3[...] = jnp.zeros_like(acc3)
    else:
        slots = tokens // 2

    slot_row = lax.broadcasted_iota(jnp.int32, (slots, tokens), 0).astype(F32)

    def masks(block):
        facts = got[block, tokens:, :].astype(F32)
        ids, slot_ids, gates = (facts[:choices, i * tokens:(i + 1) * tokens] for i in range(3))
        plain, gated = [], []
        for e in range(half):
            kept = jnp.logical_and(ids == (me * half + e).astype(F32), slot_ids >= 0.0)
            slot = jnp.sum(jnp.where(kept, slot_ids + 1.0, 0.0), axis=0, keepdims=True) - 1.0
            gate = jnp.sum(jnp.where(kept, gates, 0.0), axis=0, keepdims=True)
            hit = slot == slot_row
            plain.append(jnp.where(hit, 1.0, 0.0).astype(BF16))
            gated.append(jnp.where(hit, gate, 0.0).astype(BF16))
        return jnp.concatenate(plain, axis=0), jnp.concatenate(gated, axis=0)

    def experts_forward(mine, theirs):
        marks = [masks(block) for block in (mine, theirs)]
        placed = [mm(marks[s][0], got[block, :tokens, :]).astype(BF16) for s, block in enumerate((mine, theirs))]
        outs = []
        for e in range(half):
            rows = jnp.concatenate([part[e * slots:(e + 1) * slots] for part in placed], axis=0)
            act_1 = mm(rows, w1_ref[e]).astype(BF16).astype(F32)
            act_3 = mm(rows, w3_ref[e]).astype(BF16).astype(F32)
            hidden = (act_1 * jax.nn.sigmoid(act_1) * act_3).astype(BF16)
            outs.append(mm(hidden, w2_ref[e]).astype(BF16))

        def combine(s):
            return mm_tn(marks[s][1], jnp.concatenate([out[s * slots:(s + 1) * slots] for out in outs], axis=0))

        return combine

    def experts_backward(mine, theirs, which):
        marks = [masks(block) for block in (mine, theirs)]
        placed = [mm(marks[s][1], got[block, :tokens, :]).astype(BF16) for s, block in enumerate((mine, theirs))]
        outs = []
        for e in range(half):
            rows = saved[which, e]
            d_out = jnp.concatenate([part[e * slots:(e + 1) * slots] for part in placed], axis=0)
            pre_1 = mm(rows, w1_ref[e]).astype(BF16).astype(F32)
            pre_3 = mm(rows, w3_ref[e]).astype(BF16).astype(F32)
            sigma = jax.nn.sigmoid(pre_1)
            silu_1 = pre_1 * sigma
            hidden = (silu_1 * pre_3).astype(BF16)
            acc2[e] += mm_tn(hidden, d_out)
            grad_hid = mm_nt(d_out, w2_ref[e]).astype(BF16).astype(F32)
            grad_a1 = (grad_hid * pre_3 * sigma * (1.0 + pre_1 * (1.0 - sigma))).astype(BF16)
            grad_a3 = (grad_hid * silu_1).astype(BF16)
            acc1[e] += mm_tn(rows, grad_a1)
            acc3[e] += mm_tn(rows, grad_a3)
            outs.append((mm_nt(grad_a1, w1_ref[e]) + mm_nt(grad_a3, w3_ref[e])).astype(BF16))

        def combine(s):
            return mm_tn(marks[s][0], jnp.concatenate([out[s * slots:(s + 1) * slots] for out in outs], axis=0))

        return combine

    def send_core(step):
        which = lax.rem(step, 2)
        return remote(stage.at[which], from_core.at[which], s_core.at[which], r_core.at[which], other_core)

    def send_y(n):
        return remote(own.at[4 + n, :, first], from_y.at[n], s_y.at[n], r_y.at[n], other_y)

    def take_y(n):
        send_y(n).wait_recv()
        own[n, :, :main] += from_y[n]

    def hop(n, source, landing, base, send, recv, action):
        goal = column(n)

        @pl.when(goal > z)
        def _():
            action(remote(source, landing.at[base + goal], send, recv.at[base + goal], right))

        @pl.when(goal == z - 1)
        def _():
            action(remote(source, landing.at[base + 4], send, recv.at[base + 4], left))

        @pl.when(goal < z - 1)
        def _():
            action(remote(source, landing.at[base + goal], send, recv.at[base + goal], left))

    def chain(n, action):
        hop(n, own.at[n, :, first], from_z, 0, s_z.at[n - 1], r_z, action)

    def take_z(n, slot):
        remote(own.at[n, :, first], from_z.at[slot], s_z.at[0], r_z.at[slot], left).wait_recv()
        own[n, :, :main] += from_z[slot]

    def side_chain(across, n, action):
        hop(n, own.at[4 * across + n, :, last], side_z, 5 * across, sz_send.at[3 * across + n - 1], sz_recv, action)

    def side_take(across, n, slot):
        at_slot = 5 * across + slot
        remote(own.at[n, :, last], side_z.at[at_slot], sz_send.at[0], sz_recv.at[at_slot], left).wait_recv()
        own[4 * across + n, :, main:] += side_z[at_slot]

    def side_cross():
        return remote(own.at[4, :, last], side_y, sy_send, sy_recv, other_y)

    def at_steps(step, who, table, action):
        for when, across, n in table:
            @pl.when(jnp.logical_and(who, step == when))
            def _():
                action(across, n)

    def side_join(across, n):
        side_take(across, n, column(n))
        side_chain(across, n, start)

    def side_gather(across):
        @pl.when(z > 0)
        def _():
            side_take(across, 0, z)

        @pl.when(z < 3)
        def _():
            side_take(across, 0, 4)

    def step_body(step, carry):
        n, across = order(step)
        base = pair_base(step)
        which = lax.rem(step, 2)

        @pl.when(step == 1)
        def _():
            pass_on(1)

        @pl.when(jnp.logical_or(jnp.logical_and(step == 1, inside), jnp.logical_and(step == 2, at_end)))
        def _():
            pass_on(2)

        @pl.when(jnp.logical_or(jnp.logical_and(step == 2, inside), jnp.logical_and(step == 3, at_end)))
        def _():
            pass_on(3)

        @pl.when(jnp.logical_and(step >= 1, step <= 4))
        def _():
            block = at(column(step - 1), 1 - y, c)
            arrived(block)
            gather_to_core(3 + step, block).start()

        arrived(base + 1 - c)
        if backward:
            @pl.when(step < 7)
            def _():
                load_saved(step + 1).start()
            load_saved(step).wait()
            low, high = base, base + 1
            combine = experts_backward(low, high, which)
        else:
            low, high = base, base + 1
            combine = experts_forward(low, high)

        @pl.when(step >= 2)
        def _():
            send_core(step).wait_send()

        first, second = combine(0), combine(1)

        @pl.when(c == 0)
        def _():
            stage[which] = second
            own[across * 4 + n] = first

        @pl.when(c == 1)
        def _():
            stage[which] = first
            own[across * 4 + n] = second

        send_core(step).start()

        send_core(step).wait_recv()
        own[across * 4 + n] += from_core[which]

        @pl.when(across == 1)
        def _():
            send_y(n).start()

        at_steps(step, at_end, ((1, 0, 1), (2, 0, 2), (3, 0, 3), (4, 1, 3), (5, 1, 2), (6, 1, 1)), lambda across, n: side_chain(across, n, start))
        at_steps(step, inside, ((4, 0, 2), (5, 0, 3), (6, 0, 1), (6, 1, 3), (7, 1, 2), (7, 1, 1)), side_join)

        @pl.when(step == 6)
        def _():
            take_y(3)

            @pl.when(at_end)
            def _():
                chain(3, start)

        return carry

    lax.fori_loop(0, 8, step_body, 0)
    if backward:
        stores = [pltpu.make_async_copy(acc, ref, store_sem.at[i]) for i, (acc, ref) in enumerate(((acc1, gw1_ref), (acc2, gw2_ref), (acc3, gw3_ref)))]
        for store in stores:
            store.start()

    for n in range(4):
        along_z(n, sent)
        gather_to_y(n, me).wait_send()
    for slot in range(8):
        gather_to_core(slot, me).wait_send()
    gains = got[me, tokens:, :].astype(F32)
    attention = Attention(got, proj, ctx, x_ref, gains[choices:choices + 1], gains[choices + 1:choices + 2], head_dim)
    weights = attention.copies(wq_ref, wk_ref, wv_ref, wo_ref, att_sem)
    for copy in weights:
        copy.start()

    def join(n):
        @pl.when(inside)
        def _():
            take_z(n, column(n))
            chain(n, start)

    def pass_sum(n):
        take_y(n)

        @pl.when(at_end)
        def _():
            chain(n, start)

    if not backward:
        for copy in weights:
            copy.wait()
        attention.project()
        attention.heads()
        hid = attention.hidden()
        d_norm, gn2_ref[...] = attention.norm_pull(hid.astype(F32), attention.gain_2, du_ref[...].astype(F32))
        d_hid = (dy_ref[...].astype(F32) + d_norm.astype(F32)).astype(BF16)
        dx_ref[...] = d_hid
        for i in range(4):
            d_ctx[:, i * attention.chunk:(i + 1) * attention.chunk] = mm_nt(d_hid, attention.weight(4 + i)).astype(BF16)
        for i in range(4):
            go_ref[pl.ds(i * attention.chunk, attention.chunk), :] = mm_tn(attention.part(ctx[...], i), d_hid).astype(BF16)
    join(3)
    if backward:
        for copy in weights:
            copy.wait()
        attention.project()
    pass_sum(2)
    join(2)
    if backward:
        attention.heads()
    else:
        attention.pull_heads(d_ctx, d_proj)
    side_gather(1)
    side_cross().start()
    pass_sum(1)
    join(1)
    kv = attention.kv
    if backward:
        hid = attention.hidden()
        h_ref[...] = hid
        norm_ref[...] = attention.norm(hid.astype(F32), attention.gain_2)
    else:
        rows = attention.normed()
        for i in range(4):
            block = pl.ds(i * attention.chunk, attention.chunk)
            gq_ref[block, :] = mm_tn(attention.part(rows, i), d_proj[:, :dim]).astype(BF16)
            gk_ref[block, :] = mm_tn(attention.part(rows, i), d_proj[:, dim:dim + kv]).astype(BF16)
            gv_ref[block, :] = mm_tn(attention.part(rows, i), d_proj[:, dim + kv:]).astype(BF16)
        pulled = [mm_nt(d_proj[:, :dim], attention.weight(i)) + mm_nt(d_proj[:, dim:], attention.weight(8 + i)) for i in range(4)]
        d_rows = jnp.concatenate(pulled, axis=1).astype(BF16).astype(F32)
        d_x, gn1_ref[...] = attention.norm_pull(x_ref[...].astype(F32), attention.gain_1, d_rows)
        dx_ref[...] = (dx_ref[...].astype(F32) + d_x.astype(F32)).astype(BF16)
    side_gather(0)
    take_y(0)
    side_cross().wait_recv()
    own[0, :, main:] += side_y[...]

    @pl.when(z > 0)
    def _():
        take_z(0, z)

    @pl.when(z < 3)
    def _():
        take_z(0, 4)

    out_ref[...] = own[0].astype(out_ref.dtype)
    for n in (3, 2, 1):
        chain(n, sent)
        side_chain(0, n, sent)
        side_chain(1, n, sent)
    side_cross().wait_send()
    for n in range(4):
        send_y(n).wait_send()
    send_core(0).wait_send()
    send_core(1).wait_send()
    if backward:
        for store in stores:
            store.wait()


def exchange(backward, rows, weights, tokens, head_dim, choices, sequence, saved=None):
    w_1, w_3, w_2 = weights
    dim = rows.shape[1]
    half, ff = w_1.shape[0], w_1.shape[2]
    dma = pltpu.SemaphoreType.DMA
    block = (tokens, dim)
    model = (dim, dim)
    narrow = (dim, dim // 2)
    scratch = [
        pltpu.VMEM((tokens, 2 * dim), BF16),
        pltpu.VMEM(block, BF16),
        dma((16,)),
    ]
    if not backward:
        scratch += [pltpu.VMEM(block, BF16), pltpu.VMEM((tokens, 2 * dim), BF16)]
    scratch += [
        pltpu.VMEM((16,) + rows.shape, BF16),
        pltpu.VMEM((8,) + block, F32),
        pltpu.VMEM((2,) + block, F32),
        pltpu.VMEM((2,) + block, F32),
        pltpu.VMEM((4, tokens, dim - dim // SIDE), F32),
        pltpu.VMEM((5, tokens, dim - dim // SIDE), F32),
    ]
    tail = [pltpu.VMEM((10, tokens, dim // SIDE), F32), pltpu.VMEM((tokens, dim // SIDE), F32), dma((6,)), dma((10,)), dma(()), dma(()), dma((16,)), dma((8,)), dma((4,)), dma((5,)), dma((2,)), dma((2,)), dma((4,)), dma((4,)), dma((3,)), dma((5,))]
    any_spec = pl.BlockSpec(memory_space=pl.ANY)
    vmem_spec = pl.BlockSpec(memory_space=pltpu.VMEM)
    if backward:
        slots = saved.shape[1] // 16
        scratch += [
            pltpu.VMEM((2, half, 2 * slots, dim), BF16),
            pltpu.VMEM((half, dim, ff), F32),
            pltpu.VMEM((half, ff, dim), F32),
            pltpu.VMEM((half, dim, ff), F32),
            dma(()), dma((2,)), dma((3,)),
        ]
        operands = (rows, saved, w_1, w_3, w_2) + sequence
        in_specs = [any_spec, any_spec] + [vmem_spec] * 4 + [any_spec] * 4
        out_shape = [jax.ShapeDtypeStruct(block, BF16), jax.ShapeDtypeStruct((half, dim, ff), F32), jax.ShapeDtypeStruct((half, ff, dim), F32), jax.ShapeDtypeStruct((half, dim, ff), F32), jax.ShapeDtypeStruct(block, BF16), jax.ShapeDtypeStruct(block, BF16)]
        out_specs = [vmem_spec, any_spec, any_spec, any_spec, vmem_spec, vmem_spec]
    else:
        scratch += [dma(())]
        operands = (rows, w_1, w_3, w_2) + sequence
        in_specs = [any_spec] + [vmem_spec] * 4 + [any_spec] * 4 + [vmem_spec] * 2
        out_shape = [jax.ShapeDtypeStruct(block, F32), jax.ShapeDtypeStruct(block, BF16)]
        out_shape += [jax.ShapeDtypeStruct(shape, BF16) for shape in (model, narrow, narrow, model)]
        out_shape += [jax.ShapeDtypeStruct((1, dim), F32)] * 2
        out_specs = [vmem_spec] * 8
    return pl.pallas_call(
        functools.partial(exchange_kernel, backward, head_dim, choices),
        out_shape=out_shape,
        in_specs=in_specs,
        out_specs=out_specs,
        scratch_shapes=scratch + tail,
        name='exchange_b' if backward else 'exchange_a',
        compiler_params=pltpu.CompilerParams(collective_id=1 if backward else 0, has_side_effects=True, vmem_limit_bytes=VMEM_BYTES),
    )(*operands)


def solution(mesh):
    group = mesh.shape['expert']

    def local_step(x_a, x_b, dy_b, eid_a, slot_a, gate_a, eid_b, slot_b, gate_b, u_b, norm_1, norm_2, w_q, w_k, w_v, w_o, w_1, w_2, w_3):
        local_experts = w_1.shape[0]
        model_dim = x_a.shape[1]

        tokens = x_a.shape[0]

        def with_routing(rows, expert_ids, slot_ids, gates):
            facts = jnp.concatenate([array.astype(jnp.bfloat16).T for array in (expert_ids, slot_ids, gates)], axis=1)
            facts = jnp.pad(facts, ((0, 0), (0, model_dim - facts.shape[1])))
            table = jnp.concatenate([facts, norm_1[None], norm_2[None]], axis=0)
            table = jnp.pad(table, ((0, 16 - table.shape[0]), (0, 0)))
            return jnp.concatenate([rows, table], axis=0)

        weights = (w_1, w_3, w_2)
        head_dim = w_q.shape[2]
        layer = (w_q.reshape(model_dim, -1), w_k.reshape(model_dim, -1), w_v.reshape(model_dim, -1), w_o.reshape(-1, model_dim))
        du_rows, grad_w1, grad_w2, grad_w3, h_a, u_a = exchange(True, with_routing(dy_b, eid_b, slot_b, gate_b), weights, tokens, head_dim, eid_b.shape[1], (x_a,) + layer, u_b)
        mixed, dx_b, g_q, g_k, g_v, g_o, g_n1, g_n2 = exchange(False, with_routing(u_a, eid_a, slot_a, gate_a), weights, tokens, head_dim, eid_a.shape[1], (x_b,) + layer + (dy_b, du_rows))
        y_a = (h_a.astype(jnp.float32) + mixed).astype(jnp.bfloat16)
        g_q, g_k, g_v, g_o = (grad.astype(jnp.float32).reshape(weight.shape) for grad, weight in ((g_q, w_q), (g_k, w_k), (g_v, w_v), (g_o, w_o)))
        g_n1, g_n2 = g_n1[0], g_n2[0]
        return (y_a, dx_b, grad_w1, grad_w2, grad_w3, g_q[None], g_k[None], g_v[None], g_o[None], g_n1[None], g_n2[None])

    row_spec = P(('data', 'expert'), None)
    cube_spec = P(('data', 'expert'), None, None)
    quad_spec = P(('data', 'expert'), None, None, None)
    expert_spec = P('expert', None, None)
    in_specs = (row_spec, row_spec, row_spec, row_spec, row_spec, row_spec, row_spec, row_spec, row_spec, cube_spec, P(), P(), P(), P(), P(), P(), expert_spec, expert_spec, expert_spec)
    out_specs = (row_spec, row_spec, cube_spec, cube_spec, cube_spec, quad_spec, quad_spec, quad_spec, quad_spec, row_spec, row_spec)
    return jax.shard_map(local_step, mesh=mesh, in_specs=in_specs, out_specs=out_specs, check_vma=False)
```

```python
import functools

import jax
import jax.numpy as jnp
from jax import lax
from jax.experimental import pallas as pl
from jax.experimental.pallas import tpu as pltpu
from jax.sharding import PartitionSpec as P

F32 = jnp.float32
BF16 = jnp.bfloat16
VMEM_BYTES = 66_000_000
SIDE = 4

NORM_EPS = 1e-6


def mm(left, right):
    return lax.dot_general(left, right, (((1,), (0,)), ((), ())), preferred_element_type=F32)


def mm_nt(left, right):
    return lax.dot_general(left, right, (((1,), (1,)), ((), ())), preferred_element_type=F32)


def mm_tn(left, right):
    return lax.dot_general(left, right, (((0,), (0,)), ((), ())), preferred_element_type=F32)


class Attention:
    def __init__(self, got, proj, ctx, x_ref, gain_1, gain_2, head_dim):
        self.got, self.proj, self.ctx, self.x_ref, self.gain_1, self.gain_2 = got, proj, ctx, x_ref, gain_1, gain_2
        self.tokens, self.dim = x_ref.shape
        self.head_dim = head_dim
        self.kv = self.dim // 2
        self.chunk = self.dim // 4
        self.low = lax.broadcasted_iota(jnp.int32, (self.tokens, 2 * head_dim), 1) < head_dim
        row = lax.broadcasted_iota(jnp.int32, (2 * self.tokens, self.tokens), 0)
        row = jnp.where(row >= self.tokens, row - self.tokens, row)
        self.causal = row >= lax.broadcasted_iota(jnp.int32, (2 * self.tokens, self.tokens), 1)

    def copies(self, wq, wk, wv, wo, sems):
        n, out = self.chunk, []
        for i in range(4):
            rows = pl.ds(i * n, n)
            out.append(pltpu.make_async_copy(wq.at[rows], self.got.at[i, pl.ds(0, n)], sems.at[i]))
            out.append(pltpu.make_async_copy(wo.at[rows], self.got.at[4 + i, pl.ds(0, n)], sems.at[4 + i]))
            out.append(pltpu.make_async_copy(wk.at[rows], self.got.at[8 + i, pl.ds(0, n), pl.ds(0, self.kv)], sems.at[8 + i]))
            out.append(pltpu.make_async_copy(wv.at[rows], self.got.at[8 + i, pl.ds(0, n), pl.ds(self.kv, self.kv)], sems.at[12 + i]))
        return out

    def weight(self, i):
        return self.got[i, :self.chunk, :]

    def scale(self, wide):
        return lax.rsqrt(jnp.mean(wide * wide, axis=-1, keepdims=True) + NORM_EPS)

    def norm(self, wide, gain):
        return (wide * self.scale(wide) * gain).astype(BF16)

    def norm_pull(self, wide, gain, grad):
        inv = self.scale(wide)
        gain_grad = jnp.sum(grad * (wide * inv), axis=0, keepdims=True).astype(BF16).astype(F32)
        inner = grad * gain
        row_grad = inv * inner - wide * (inv * inv * inv * jnp.mean(inner * wide, axis=-1, keepdims=True))
        return row_grad.astype(BF16), gain_grad

    def normed(self):
        return self.norm(self.x_ref[...].astype(F32), self.gain_1)

    def part(self, rows, i):
        return rows[:, i * self.chunk:(i + 1) * self.chunk]

    def project(self):
        rows = self.normed()
        self.proj[:, :self.dim] = sum(mm(self.part(rows, i), self.weight(i)) for i in range(4)).astype(BF16)
        self.proj[:, self.dim:] = sum(mm(self.part(rows, i), self.weight(8 + i)) for i in range(4)).astype(BF16)

    def stacked(self, ref, start):
        pair = ref[:, pl.ds(start, 2 * self.head_dim)].astype(F32)
        return jnp.concatenate([jnp.where(self.low, pair, 0.0), jnp.where(self.low, 0.0, pair)], axis=0).astype(BF16)

    def doubled(self, start, odd):
        pair = self.proj[:, pl.ds(start, 2 * self.head_dim)].astype(F32)
        turned = pltpu.roll(pair, self.head_dim, 1)
        return (jnp.where(self.low, turned, pair) if odd else jnp.where(self.low, pair, turned)).astype(BF16)

    def merged(self, both):
        return jnp.where(self.low, both[:self.tokens], both[self.tokens:])

    def group(self, quad, odd):
        width = 2 * self.head_dim
        at = pl.multiple_of((2 * quad + odd) * width, width)
        kv_at = pl.multiple_of(quad * width, width)
        query = self.stacked(self.proj, at)
        keys = self.doubled(self.dim + kv_at, odd)
        vals = self.doubled(self.dim + self.kv + kv_at, odd)
        scores = jnp.where(self.causal, mm_nt(query, keys) * self.head_dim ** -0.5, -1e30)
        powers = jnp.exp(scores - jnp.max(scores, axis=-1, keepdims=True))
        return at, kv_at, query, keys, vals, powers / jnp.sum(powers, axis=-1, keepdims=True)

    def heads(self):
        def body(quad, carry):
            for odd in range(2):
                at, _, _, _, vals, probs = self.group(quad, odd)
                self.ctx[:, pl.ds(at, 2 * self.head_dim)] = self.merged(mm(probs.astype(BF16), vals)).astype(BF16)
            return carry

        lax.fori_loop(0, self.kv // (2 * self.head_dim), body, 0)

    def hidden(self):
        attn = sum(mm(self.part(self.ctx[...], i), self.weight(4 + i)) for i in range(4)).astype(BF16)
        return (self.x_ref[...].astype(F32) + attn.astype(F32)).astype(BF16)

    def pull_heads(self, d_ctx, d_proj):
        def fold(both):
            return both + pltpu.roll(both, self.head_dim, 1)

        def body(quad, carry):
            d_keys, d_vals = [], []
            for odd in range(2):
                at, kv_at, query, keys, vals, probs = self.group(quad, odd)
                grad = self.stacked(d_ctx, at)
                d_probs = mm_nt(grad, vals).astype(BF16).astype(F32)
                d_vals.append(fold(mm_tn(probs.astype(BF16), grad)))
                d_scores = probs * (d_probs - jnp.sum(probs * d_probs, axis=-1, keepdims=True))
                d_scores = (jnp.where(self.causal, d_scores, 0.0) * self.head_dim ** -0.5).astype(BF16)
                d_proj[:, pl.ds(at, 2 * self.head_dim)] = self.merged(mm(d_scores, keys)).astype(BF16)
                d_keys.append(fold(mm_tn(d_scores, query)))
            d_proj[:, pl.ds(self.dim + kv_at, 2 * self.head_dim)] = jnp.where(self.low, d_keys[0], d_keys[1]).astype(BF16)
            d_proj[:, pl.ds(self.dim + self.kv + kv_at, 2 * self.head_dim)] = jnp.where(self.low, d_vals[0], d_vals[1]).astype(BF16)
            return carry

        lax.fori_loop(0, self.kv // (2 * self.head_dim), body, 0)


def exchange_kernel(backward, head_dim, choices, *refs):
    if backward:
        (rows_ref, u_ref, w1_ref, w3_ref, w2_ref, x_ref, wq_ref, wk_ref, wv_ref, wo_ref,
         out_ref, gw1_ref, gw2_ref, gw3_ref, h_ref, norm_ref, proj, ctx, att_sem, got, own, stage, from_core, from_y, from_z, saved, acc1, acc2, acc3,
         own_sem, load_sem, store_sem, side_z, side_y, sz_send, sz_recv, sy_send, sy_recv, g_recv, g_core, g_y, g_z, s_core, r_core, s_y, r_y, s_z, r_z) = refs
    else:
        (rows_ref, w1_ref, w3_ref, w2_ref, x_ref, wq_ref, wk_ref, wv_ref, wo_ref, dy_ref, du_ref,
         out_ref, dx_ref, gq_ref, gk_ref, gv_ref, go_ref, gn1_ref, gn2_ref, proj, ctx, att_sem, d_ctx, d_proj, mats, got, own, stage, from_core, from_y, from_z,
         own_sem, side_z, side_y, sz_send, sz_recv, sy_send, sy_recv, g_recv, g_core, g_y, g_z, s_core, r_core, s_y, r_y, s_z, r_z) = refs
    tokens, dim = own.shape[1], own.shape[2]
    half = w1_ref.shape[0]
    main = dim - dim // SIDE
    first, last = pl.ds(0, main), pl.ds(main, dim - main)
    me = lax.axis_index('expert')
    z, y, c = lax.div(me, 4), lax.rem(lax.div(me, 2), 2), lax.rem(me, 2)

    def at(zz, yy, cc):
        return (zz * 2 + yy) * 2 + cc

    other_core = at(z, y, 1 - c)
    other_y = at(z, 1 - y, c)

    upper, odd = lax.div(z, 2), lax.rem(z, 2)
    at_end = jnp.logical_or(z == 0, z == 3)
    inside = jnp.logical_and(z > 0, z < 3)

    def column(n):
        far = lax.div(n, 2)
        return far * (n + upper * (3 - 2 * n)) + (1 - far) * (2 * upper + lax.rem(odd + n, 2))

    right, left = at(lax.rem(z + 1, 4), y, c), at(lax.rem(z + 3, 4), y, c)

    def remote(src, dst, send, recv, peer):
        return pltpu.make_async_remote_copy(src_ref=src, dst_ref=dst, send_sem=send, recv_sem=recv, device_id={'expert': peer}, device_id_type=pl.DeviceIdType.MESH)

    barrier = pltpu.get_barrier_semaphore()
    for peer in (other_core, other_y, right, left):
        pl.semaphore_signal(barrier, inc=1, device_id={'expert': peer}, device_id_type=pl.DeviceIdType.MESH)
    load_own = pltpu.make_async_copy(rows_ref, got.at[me], own_sem)
    load_own.start()
    pl.semaphore_wait(barrier, 4)
    load_own.wait()

    def gather_to_core(slot, block):
        return remote(got.at[block], got.at[block], g_core.at[slot], g_recv.at[block], other_core)

    def gather_to_y(n, block):
        return remote(got.at[block], got.at[block], g_y.at[n], g_recv.at[block], other_y)

    def gather_along(sem, block, peer):
        return remote(got.at[block], got.at[block], g_z.at[sem], g_recv.at[block], peer)

    def arrived(block):
        remote(got.at[block], got.at[block], g_core.at[0], g_recv.at[block], other_core).wait_recv()

    def along_z(n, action):
        source = column(n)
        block = at(source, y, c)

        @pl.when(jnp.logical_and(source <= z, z < 3))
        def _():
            action(gather_along(n, block, right))

        @pl.when(jnp.logical_and(source >= z, z > 0))
        def _():
            action(gather_along(n if n else 4, block, left))

    def start(copy):
        copy.start()

    def sent(copy):
        copy.wait_send()

    along_z(0, start)
    gather_to_y(0, me).start()
    gather_to_core(0, me).start()
    gains = got[me, tokens:, :].astype(F32)
    attention = Attention(got if backward else mats, proj, ctx, x_ref, gains[choices:choices + 1], gains[choices + 1:choices + 2], head_dim)
    weights = attention.copies(wq_ref, wk_ref, wv_ref, wo_ref, att_sem)
    if not backward:
        for copy in weights:
            copy.start()

    def pass_on(n):
        block = at(column(n), y, c)
        arrived(block)
        along_z(n, start)
        gather_to_y(n, block).start()
        gather_to_core(n, block).start()

    def order(step):
        late = lax.div(step, 4)
        return step + late * (7 - 2 * step), late

    def pair_base(step):
        n, across = order(step)
        return at(column(n), lax.rem(y + across, 2), 0)

    if backward:
        slots = saved.shape[2] // 2

        def load_saved(step):
            start = pl.multiple_of(pair_base(step) * slots, 2 * slots)
            which = lax.rem(step, 2)
            return pltpu.make_async_copy(u_ref.at[:, pl.ds(start, 2 * slots), :], saved.at[which], load_sem.at[which])

        load_saved(0).start()
        acc1[...] = jnp.zeros_like(acc1)
        acc2[...] = jnp.zeros_like(acc2)
        acc3[...] = jnp.zeros_like(acc3)
    else:
        slots = tokens // 2

    slot_row = lax.broadcasted_iota(jnp.int32, (slots, tokens), 0).astype(F32)

    def masks(block):
        facts = got[block, tokens:, :].astype(F32)
        ids, slot_ids, gates = (facts[:choices, i * tokens:(i + 1) * tokens] for i in range(3))
        plain, gated = [], []
        for e in range(half):
            kept = jnp.logical_and(ids == (me * half + e).astype(F32), slot_ids >= 0.0)
            slot = jnp.sum(jnp.where(kept, slot_ids + 1.0, 0.0), axis=0, keepdims=True) - 1.0
            gate = jnp.sum(jnp.where(kept, gates, 0.0), axis=0, keepdims=True)
            hit = slot == slot_row
            plain.append(jnp.where(hit, 1.0, 0.0).astype(BF16))
            gated.append(jnp.where(hit, gate, 0.0).astype(BF16))
        return jnp.concatenate(plain, axis=0), jnp.concatenate(gated, axis=0)

    def experts_forward(mine, theirs):
        marks = [masks(block) for block in (mine, theirs)]
        placed = [mm(marks[s][0], got[block, :tokens, :]).astype(BF16) for s, block in enumerate((mine, theirs))]
        outs = []
        for e in range(half):
            rows = jnp.concatenate([part[e * slots:(e + 1) * slots] for part in placed], axis=0)
            act_1 = mm(rows, w1_ref[e]).astype(BF16).astype(F32)
            act_3 = mm(rows, w3_ref[e]).astype(BF16).astype(F32)
            hidden = (act_1 * jax.nn.sigmoid(act_1) * act_3).astype(BF16)
            outs.append(mm(hidden, w2_ref[e]).astype(BF16))

        def combine(s):
            return mm_tn(marks[s][1], jnp.concatenate([out[s * slots:(s + 1) * slots] for out in outs], axis=0))

        return combine

    def experts_backward(mine, theirs, which):
        marks = [masks(block) for block in (mine, theirs)]
        placed = [mm(marks[s][1], got[block, :tokens, :]).astype(BF16) for s, block in enumerate((mine, theirs))]
        outs = []
        for e in range(half):
            rows = saved[which, e]
            d_out = jnp.concatenate([part[e * slots:(e + 1) * slots] for part in placed], axis=0)
            pre_1 = mm(rows, w1_ref[e]).astype(BF16).astype(F32)
            pre_3 = mm(rows, w3_ref[e]).astype(BF16).astype(F32)
            sigma = jax.nn.sigmoid(pre_1)
            silu_1 = pre_1 * sigma
            hidden = (silu_1 * pre_3).astype(BF16)
            acc2[e] += mm_tn(hidden, d_out)
            grad_hid = mm_nt(d_out, w2_ref[e]).astype(BF16).astype(F32)
            grad_a1 = (grad_hid * pre_3 * sigma * (1.0 + pre_1 * (1.0 - sigma))).astype(BF16)
            grad_a3 = (grad_hid * silu_1).astype(BF16)
            acc1[e] += mm_tn(rows, grad_a1)
            acc3[e] += mm_tn(rows, grad_a3)
            outs.append((mm_nt(grad_a1, w1_ref[e]) + mm_nt(grad_a3, w3_ref[e])).astype(BF16))

        def combine(s):
            return mm_tn(marks[s][0], jnp.concatenate([out[s * slots:(s + 1) * slots] for out in outs], axis=0))

        return combine

    def send_core(step):
        which = lax.rem(step, 2)
        return remote(stage.at[which], from_core.at[which], s_core.at[which], r_core.at[which], other_core)

    def send_y(n):
        return remote(own.at[4 + n, :, first], from_y.at[n], s_y.at[n], r_y.at[n], other_y)

    def take_y(n):
        send_y(n).wait_recv()
        own[n, :, :main] += from_y[n]

    def hop(n, source, landing, base, send, recv, action):
        goal = column(n)

        @pl.when(goal > z)
        def _():
            action(remote(source, landing.at[base + goal], send, recv.at[base + goal], right))

        @pl.when(goal == z - 1)
        def _():
            action(remote(source, landing.at[base + 4], send, recv.at[base + 4], left))

        @pl.when(goal < z - 1)
        def _():
            action(remote(source, landing.at[base + goal], send, recv.at[base + goal], left))

    def chain(n, action):
        hop(n, own.at[n, :, first], from_z, 0, s_z.at[n - 1], r_z, action)

    def take_z(n, slot):
        remote(own.at[n, :, first], from_z.at[slot], s_z.at[0], r_z.at[slot], left).wait_recv()
        own[n, :, :main] += from_z[slot]

    def side_chain(across, n, action):
        hop(n, own.at[4 * across + n, :, last], side_z, 5 * across, sz_send.at[3 * across + n - 1], sz_recv, action)

    def side_take(across, n, slot):
        at_slot = 5 * across + slot
        remote(own.at[n, :, last], side_z.at[at_slot], sz_send.at[0], sz_recv.at[at_slot], left).wait_recv()
        own[4 * across + n, :, main:] += side_z[at_slot]

    def side_cross():
        return remote(own.at[4, :, last], side_y, sy_send, sy_recv, other_y)

    def at_steps(step, who, table, action):
        for when, across, n in table:
            @pl.when(jnp.logical_and(who, step == when))
            def _():
                action(across, n)

    def side_join(across, n):
        side_take(across, n, column(n))
        side_chain(across, n, start)

    def side_gather(across):
        @pl.when(z > 0)
        def _():
            side_take(across, 0, z)

        @pl.when(z < 3)
        def _():
            side_take(across, 0, 4)

    def step_body(step, carry):
        n, across = order(step)
        base = pair_base(step)
        which = lax.rem(step, 2)

        @pl.when(step == 1)
        def _():
            pass_on(1)

        @pl.when(jnp.logical_or(jnp.logical_and(step == 1, inside), jnp.logical_and(step == 2, at_end)))
        def _():
            pass_on(2)

        @pl.when(jnp.logical_or(jnp.logical_and(step == 2, inside), jnp.logical_and(step == 3, at_end)))
        def _():
            pass_on(3)

        @pl.when(jnp.logical_and(step >= 1, step <= 4))
        def _():
            block = at(column(step - 1), 1 - y, c)
            arrived(block)
            gather_to_core(3 + step, block).start()

        arrived(base + 1 - c)
        if backward:
            @pl.when(step < 7)
            def _():
                load_saved(step + 1).start()
            load_saved(step).wait()
            low, high = base, base + 1
            combine = experts_backward(low, high, which)
        else:
            low, high = base, base + 1
            combine = experts_forward(low, high)

        @pl.when(step >= 2)
        def _():
            send_core(step).wait_send()

        first, second = combine(0), combine(1)

        @pl.when(c == 0)
        def _():
            stage[which] = second
            own[across * 4 + n] = first

        @pl.when(c == 1)
        def _():
            stage[which] = first
            own[across * 4 + n] = second

        send_core(step).start()

        send_core(step).wait_recv()
        own[across * 4 + n] += from_core[which]

        @pl.when(across == 1)
        def _():
            send_y(n).start()

        at_steps(step, at_end, ((1, 0, 1), (2, 0, 2), (3, 0, 3), (4, 1, 3), (5, 1, 2), (6, 1, 1)), lambda across, n: side_chain(across, n, start))
        at_steps(step, inside, ((4, 0, 2), (5, 0, 3), (6, 0, 1), (6, 1, 3), (7, 1, 2), (7, 1, 1)), side_join)

        if not backward:
            @pl.when(step == 1)
            def _():
                attention.heads()

            @pl.when(step == 2)
            def _():
                pull_output()

        @pl.when(step == 6)
        def _():
            take_y(3)

            @pl.when(at_end)
            def _():
                chain(3, start)

        return carry

    def pull_output():
        hid = attention.hidden()
        d_norm, gn2_ref[...] = attention.norm_pull(hid.astype(F32), attention.gain_2, du_ref[...].astype(F32))
        d_hid = (dy_ref[...].astype(F32) + d_norm.astype(F32)).astype(BF16)
        dx_ref[...] = d_hid
        for i in range(4):
            d_ctx[:, i * attention.chunk:(i + 1) * attention.chunk] = mm_nt(d_hid, attention.weight(4 + i)).astype(BF16)
        for i in range(4):
            go_ref[pl.ds(i * attention.chunk, attention.chunk), :] = mm_tn(attention.part(ctx[...], i), d_hid).astype(BF16)

    if not backward:
        for copy in weights:
            copy.wait()
        attention.project()
    lax.fori_loop(0, 8, step_body, 0)
    if backward:
        stores = [pltpu.make_async_copy(acc, ref, store_sem.at[i]) for i, (acc, ref) in enumerate(((acc1, gw1_ref), (acc2, gw2_ref), (acc3, gw3_ref)))]
        for store in stores:
            store.start()

    for n in range(4):
        along_z(n, sent)
        gather_to_y(n, me).wait_send()
    for slot in range(8):
        gather_to_core(slot, me).wait_send()
    if backward:
        for copy in weights:
            copy.start()

    def join(n):
        @pl.when(inside)
        def _():
            take_z(n, column(n))
            chain(n, start)

    def pass_sum(n):
        take_y(n)

        @pl.when(at_end)
        def _():
            chain(n, start)

    join(3)
    pass_sum(2)
    if backward:
        for copy in weights:
            copy.wait()
        attention.project()
        attention.heads()
    else:
        attention.pull_heads(d_ctx, d_proj)
    join(2)
    side_gather(1)
    side_cross().start()
    pass_sum(1)
    kv = attention.kv
    if backward:
        hid = attention.hidden()
        h_ref[...] = hid
        norm_ref[...] = attention.norm(hid.astype(F32), attention.gain_2)
    else:
        rows = attention.normed()
        for i in range(4):
            block = pl.ds(i * attention.chunk, attention.chunk)
            gq_ref[block, :] = mm_tn(attention.part(rows, i), d_proj[:, :dim]).astype(BF16)
            gk_ref[block, :] = mm_tn(attention.part(rows, i), d_proj[:, dim:dim + kv]).astype(BF16)
            gv_ref[block, :] = mm_tn(attention.part(rows, i), d_proj[:, dim + kv:]).astype(BF16)
    join(1)
    if not backward:
        pulled = [mm_nt(d_proj[:, :dim], attention.weight(i)) + mm_nt(d_proj[:, dim:], attention.weight(8 + i)) for i in range(4)]
        d_rows = jnp.concatenate(pulled, axis=1).astype(BF16).astype(F32)
        d_x, gn1_ref[...] = attention.norm_pull(x_ref[...].astype(F32), attention.gain_1, d_rows)
        dx_ref[...] = (dx_ref[...].astype(F32) + d_x.astype(F32)).astype(BF16)
    side_gather(0)
    take_y(0)
    side_cross().wait_recv()
    own[0, :, main:] += side_y[...]

    @pl.when(z > 0)
    def _():
        take_z(0, z)

    @pl.when(z < 3)
    def _():
        take_z(0, 4)

    out_ref[...] = own[0].astype(out_ref.dtype)
    for n in (3, 2, 1):
        chain(n, sent)
        side_chain(0, n, sent)
        side_chain(1, n, sent)
    side_cross().wait_send()
    for n in range(4):
        send_y(n).wait_send()
    send_core(0).wait_send()
    send_core(1).wait_send()
    if backward:
        for store in stores:
            store.wait()


def exchange(backward, rows, weights, tokens, head_dim, choices, sequence, saved=None):
    w_1, w_3, w_2 = weights
    dim = rows.shape[1]
    half, ff = w_1.shape[0], w_1.shape[2]
    dma = pltpu.SemaphoreType.DMA
    block = (tokens, dim)
    model = (dim, dim)
    narrow = (dim, dim // 2)
    scratch = [
        pltpu.VMEM((tokens, 2 * dim), BF16),
        pltpu.VMEM(block, BF16),
        dma((16,)),
    ]
    if not backward:
        scratch += [pltpu.VMEM(block, BF16), pltpu.VMEM((tokens, 2 * dim), BF16), pltpu.VMEM((12, dim // 4, dim), BF16)]
    scratch += [
        pltpu.VMEM((16,) + rows.shape, BF16),
        pltpu.VMEM((8,) + block, F32),
        pltpu.VMEM((2,) + block, F32),
        pltpu.VMEM((2,) + block, F32),
        pltpu.VMEM((4, tokens, dim - dim // SIDE), F32),
        pltpu.VMEM((5, tokens, dim - dim // SIDE), F32),
    ]
    tail = [pltpu.VMEM((10, tokens, dim // SIDE), F32), pltpu.VMEM((tokens, dim // SIDE), F32), dma((6,)), dma((10,)), dma(()), dma(()), dma((16,)), dma((8,)), dma((4,)), dma((5,)), dma((2,)), dma((2,)), dma((4,)), dma((4,)), dma((3,)), dma((5,))]
    any_spec = pl.BlockSpec(memory_space=pl.ANY)
    vmem_spec = pl.BlockSpec(memory_space=pltpu.VMEM)
    if backward:
        slots = saved.shape[1] // 16
        scratch += [
            pltpu.VMEM((2, half, 2 * slots, dim), BF16),
            pltpu.VMEM((half, dim, ff), F32),
            pltpu.VMEM((half, ff, dim), F32),
            pltpu.VMEM((half, dim, ff), F32),
            dma(()), dma((2,)), dma((3,)),
        ]
        operands = (rows, saved, w_1, w_3, w_2) + sequence
        in_specs = [any_spec, any_spec] + [vmem_spec] * 4 + [any_spec] * 4
        out_shape = [jax.ShapeDtypeStruct(block, BF16), jax.ShapeDtypeStruct((half, dim, ff), F32), jax.ShapeDtypeStruct((half, ff, dim), F32), jax.ShapeDtypeStruct((half, dim, ff), F32), jax.ShapeDtypeStruct(block, BF16), jax.ShapeDtypeStruct(block, BF16)]
        out_specs = [vmem_spec, any_spec, any_spec, any_spec, vmem_spec, vmem_spec]
    else:
        scratch += [dma(())]
        operands = (rows, w_1, w_3, w_2) + sequence
        in_specs = [any_spec] + [vmem_spec] * 4 + [any_spec] * 4 + [vmem_spec] * 2
        out_shape = [jax.ShapeDtypeStruct(block, F32), jax.ShapeDtypeStruct(block, BF16)]
        out_shape += [jax.ShapeDtypeStruct(shape, BF16) for shape in (model, narrow, narrow, model)]
        out_shape += [jax.ShapeDtypeStruct((1, dim), F32)] * 2
        out_specs = [vmem_spec] * 8
    return pl.pallas_call(
        functools.partial(exchange_kernel, backward, head_dim, choices),
        out_shape=out_shape,
        in_specs=in_specs,
        out_specs=out_specs,
        scratch_shapes=scratch + tail,
        name='exchange_b' if backward else 'exchange_a',
        compiler_params=pltpu.CompilerParams(collective_id=1 if backward else 0, has_side_effects=True, vmem_limit_bytes=VMEM_BYTES),
    )(*operands)


def solution(mesh):
    group = mesh.shape['expert']

    def local_step(x_a, x_b, dy_b, eid_a, slot_a, gate_a, eid_b, slot_b, gate_b, u_b, norm_1, norm_2, w_q, w_k, w_v, w_o, w_1, w_2, w_3):
        local_experts = w_1.shape[0]
        model_dim = x_a.shape[1]

        tokens = x_a.shape[0]

        def with_routing(rows, expert_ids, slot_ids, gates):
            facts = jnp.concatenate([array.astype(jnp.bfloat16).T for array in (expert_ids, slot_ids, gates)], axis=1)
            facts = jnp.pad(facts, ((0, 0), (0, model_dim - facts.shape[1])))
            table = jnp.concatenate([facts, norm_1[None], norm_2[None]], axis=0)
            table = jnp.pad(table, ((0, 16 - table.shape[0]), (0, 0)))
            return jnp.concatenate([rows, table], axis=0)

        weights = (w_1, w_3, w_2)
        head_dim = w_q.shape[2]
        layer = (w_q.reshape(model_dim, -1), w_k.reshape(model_dim, -1), w_v.reshape(model_dim, -1), w_o.reshape(-1, model_dim))
        du_rows, grad_w1, grad_w2, grad_w3, h_a, u_a = exchange(True, with_routing(dy_b, eid_b, slot_b, gate_b), weights, tokens, head_dim, eid_b.shape[1], (x_a,) + layer, u_b)
        mixed, dx_b, g_q, g_k, g_v, g_o, g_n1, g_n2 = exchange(False, with_routing(u_a, eid_a, slot_a, gate_a), weights, tokens, head_dim, eid_a.shape[1], (x_b,) + layer + (dy_b, du_rows))
        y_a = (h_a.astype(jnp.float32) + mixed).astype(jnp.bfloat16)
        g_q, g_k, g_v, g_o = (grad.astype(jnp.float32).reshape(weight.shape) for grad, weight in ((g_q, w_q), (g_k, w_k), (g_v, w_v), (g_o, w_o)))
        g_n1, g_n2 = g_n1[0], g_n2[0]
        return (y_a, dx_b, grad_w1, grad_w2, grad_w3, g_q[None], g_k[None], g_v[None], g_o[None], g_n1[None], g_n2[None])

    row_spec = P(('data', 'expert'), None)
    cube_spec = P(('data', 'expert'), None, None)
    quad_spec = P(('data', 'expert'), None, None, None)
    expert_spec = P('expert', None, None)
    in_specs = (row_spec, row_spec, row_spec, row_spec, row_spec, row_spec, row_spec, row_spec, row_spec, cube_spec, P(), P(), P(), P(), P(), P(), expert_spec, expert_spec, expert_spec)
    out_specs = (row_spec, row_spec, cube_spec, cube_spec, cube_spec, quad_spec, quad_spec, quad_spec, quad_spec, row_spec, row_spec)
    return jax.shard_map(local_step, mesh=mesh, in_specs=in_specs, out_specs=out_specs, check_vma=False)
```

```python
import functools

import jax
import jax.numpy as jnp
from jax import lax
from jax.experimental import pallas as pl
from jax.experimental.pallas import tpu as pltpu
from jax.sharding import PartitionSpec as P

F32 = jnp.float32
BF16 = jnp.bfloat16
VMEM_BYTES = 66_000_000
SIDE = 4

NORM_EPS = 1e-6


def mm(left, right):
    return lax.dot_general(left, right, (((1,), (0,)), ((), ())), preferred_element_type=F32)


def mm_nt(left, right):
    return lax.dot_general(left, right, (((1,), (1,)), ((), ())), preferred_element_type=F32)


def mm_tn(left, right):
    return lax.dot_general(left, right, (((0,), (0,)), ((), ())), preferred_element_type=F32)


class Attention:
    def __init__(self, got, proj, ctx, x_ref, gain_1, gain_2, head_dim):
        self.got, self.proj, self.ctx, self.x_ref, self.gain_1, self.gain_2 = got, proj, ctx, x_ref, gain_1, gain_2
        self.tokens, self.dim = x_ref.shape
        self.head_dim = head_dim
        self.kv = self.dim // 2
        self.chunk = self.dim // 4
        self.low = lax.broadcasted_iota(jnp.int32, (self.tokens, 2 * head_dim), 1) < head_dim
        row = lax.broadcasted_iota(jnp.int32, (2 * self.tokens, self.tokens), 0)
        row = jnp.where(row >= self.tokens, row - self.tokens, row)
        self.causal = row >= lax.broadcasted_iota(jnp.int32, (2 * self.tokens, self.tokens), 1)

    def copies(self, wq, wk, wv, wo, sems):
        n, out = self.chunk, []
        for i in range(4):
            rows = pl.ds(i * n, n)
            out.append(pltpu.make_async_copy(wq.at[rows], self.got.at[i, pl.ds(0, n)], sems.at[i]))
            out.append(pltpu.make_async_copy(wo.at[rows], self.got.at[4 + i, pl.ds(0, n)], sems.at[4 + i]))
            out.append(pltpu.make_async_copy(wk.at[rows], self.got.at[8 + i, pl.ds(0, n), pl.ds(0, self.kv)], sems.at[8 + i]))
            out.append(pltpu.make_async_copy(wv.at[rows], self.got.at[8 + i, pl.ds(0, n), pl.ds(self.kv, self.kv)], sems.at[12 + i]))
        return out

    def weight(self, i):
        return self.got[i, :self.chunk, :]

    def scale(self, wide):
        return lax.rsqrt(jnp.mean(wide * wide, axis=-1, keepdims=True) + NORM_EPS)

    def norm(self, wide, gain):
        return (wide * self.scale(wide) * gain).astype(BF16)

    def norm_pull(self, wide, gain, grad):
        inv = self.scale(wide)
        gain_grad = jnp.sum(grad * (wide * inv), axis=0, keepdims=True).astype(BF16).astype(F32)
        inner = grad * gain
        row_grad = inv * inner - wide * (inv * inv * inv * jnp.mean(inner * wide, axis=-1, keepdims=True))
        return row_grad.astype(BF16), gain_grad

    def normed(self):
        return self.norm(self.x_ref[...].astype(F32), self.gain_1)

    def part(self, rows, i):
        return rows[:, i * self.chunk:(i + 1) * self.chunk]

    def project(self):
        rows = self.normed()
        self.proj[:, :self.dim] = sum(mm(self.part(rows, i), self.weight(i)) for i in range(4)).astype(BF16)
        self.proj[:, self.dim:] = sum(mm(self.part(rows, i), self.weight(8 + i)) for i in range(4)).astype(BF16)

    def stacked(self, ref, start):
        pair = ref[:, pl.ds(start, 2 * self.head_dim)].astype(F32)
        return jnp.concatenate([jnp.where(self.low, pair, 0.0), jnp.where(self.low, 0.0, pair)], axis=0).astype(BF16)

    def doubled(self, start, odd):
        pair = self.proj[:, pl.ds(start, 2 * self.head_dim)].astype(F32)
        turned = pltpu.roll(pair, self.head_dim, 1)
        return (jnp.where(self.low, turned, pair) if odd else jnp.where(self.low, pair, turned)).astype(BF16)

    def merged(self, both):
        return jnp.where(self.low, both[:self.tokens], both[self.tokens:])

    def group(self, quad, odd):
        width = 2 * self.head_dim
        at = pl.multiple_of((2 * quad + odd) * width, width)
        kv_at = pl.multiple_of(quad * width, width)
        query = self.stacked(self.proj, at)
        keys = self.doubled(self.dim + kv_at, odd)
        vals = self.doubled(self.dim + self.kv + kv_at, odd)
        scores = jnp.where(self.causal, mm_nt(query, keys) * self.head_dim ** -0.5, -1e30)
        powers = jnp.exp(scores - jnp.max(scores, axis=-1, keepdims=True))
        return at, kv_at, query, keys, vals, powers / jnp.sum(powers, axis=-1, keepdims=True)

    def heads(self):
        def body(quad, carry):
            for odd in range(2):
                at, _, _, _, vals, probs = self.group(quad, odd)
                self.ctx[:, pl.ds(at, 2 * self.head_dim)] = self.merged(mm(probs.astype(BF16), vals)).astype(BF16)
            return carry

        lax.fori_loop(0, self.kv // (2 * self.head_dim), body, 0)

    def hidden(self):
        attn = sum(mm(self.part(self.ctx[...], i), self.weight(4 + i)) for i in range(4)).astype(BF16)
        return (self.x_ref[...].astype(F32) + attn.astype(F32)).astype(BF16)

    def pull_heads(self, d_ctx, d_proj):
        def fold(both):
            return both + pltpu.roll(both, self.head_dim, 1)

        def body(quad, carry):
            d_keys, d_vals = [], []
            for odd in range(2):
                at, kv_at, query, keys, vals, probs = self.group(quad, odd)
                grad = self.stacked(d_ctx, at)
                d_probs = mm_nt(grad, vals).astype(BF16).astype(F32)
                d_vals.append(fold(mm_tn(probs.astype(BF16), grad)))
                d_scores = probs * (d_probs - jnp.sum(probs * d_probs, axis=-1, keepdims=True))
                d_scores = (jnp.where(self.causal, d_scores, 0.0) * self.head_dim ** -0.5).astype(BF16)
                d_proj[:, pl.ds(at, 2 * self.head_dim)] = self.merged(mm(d_scores, keys)).astype(BF16)
                d_keys.append(fold(mm_tn(d_scores, query)))
            d_proj[:, pl.ds(self.dim + kv_at, 2 * self.head_dim)] = jnp.where(self.low, d_keys[0], d_keys[1]).astype(BF16)
            d_proj[:, pl.ds(self.dim + self.kv + kv_at, 2 * self.head_dim)] = jnp.where(self.low, d_vals[0], d_vals[1]).astype(BF16)
            return carry

        lax.fori_loop(0, self.kv // (2 * self.head_dim), body, 0)


def exchange_kernel(backward, head_dim, choices, *refs):
    if backward:
        (rows_ref, u_ref, w1_ref, w3_ref, w2_ref, x_ref, wq_ref, wk_ref, wv_ref, wo_ref,
         out_ref, gw1_ref, gw2_ref, gw3_ref, h_ref, norm_ref, proj, ctx, att_sem, got, own, stage, from_core, from_y, from_z, saved, acc1, acc2, acc3,
         own_sem, load_sem, store_sem, side_z, side_y, sz_send, sz_recv, sy_send, sy_recv, g_recv, g_core, g_y, g_z, s_core, r_core, s_y, r_y, s_z, r_z) = refs
    else:
        (rows_ref, w1_ref, w3_ref, w2_ref, x_ref, wq_ref, wk_ref, wv_ref, wo_ref, dy_ref, du_ref, base_ref,
         out_ref, dx_ref, gq_ref, gk_ref, gv_ref, go_ref, gn1_ref, gn2_ref, proj, ctx, att_sem, d_ctx, d_proj, mats, got, own, stage, from_core, from_y, from_z,
         own_sem, side_z, side_y, sz_send, sz_recv, sy_send, sy_recv, g_recv, g_core, g_y, g_z, s_core, r_core, s_y, r_y, s_z, r_z) = refs
    tokens, dim = own.shape[1], own.shape[2]
    half = w1_ref.shape[0]
    main = dim - dim // SIDE
    first, last = pl.ds(0, main), pl.ds(main, dim - main)
    me = lax.axis_index('expert')
    z, y, c = lax.div(me, 4), lax.rem(lax.div(me, 2), 2), lax.rem(me, 2)

    def at(zz, yy, cc):
        return (zz * 2 + yy) * 2 + cc

    other_core = at(z, y, 1 - c)
    other_y = at(z, 1 - y, c)

    upper, odd = lax.div(z, 2), lax.rem(z, 2)
    at_end = jnp.logical_or(z == 0, z == 3)
    inside = jnp.logical_and(z > 0, z < 3)

    def column(n):
        far = lax.div(n, 2)
        return far * (n + upper * (3 - 2 * n)) + (1 - far) * (2 * upper + lax.rem(odd + n, 2))

    right, left = at(lax.rem(z + 1, 4), y, c), at(lax.rem(z + 3, 4), y, c)

    def remote(src, dst, send, recv, peer):
        return pltpu.make_async_remote_copy(src_ref=src, dst_ref=dst, send_sem=send, recv_sem=recv, device_id={'expert': peer}, device_id_type=pl.DeviceIdType.MESH)

    barrier = pltpu.get_barrier_semaphore()
    for peer in (other_core, other_y, right, left):
        pl.semaphore_signal(barrier, inc=1, device_id={'expert': peer}, device_id_type=pl.DeviceIdType.MESH)
    load_own = pltpu.make_async_copy(rows_ref, got.at[me], own_sem)
    load_own.start()
    pl.semaphore_wait(barrier, 4)
    load_own.wait()

    def gather_to_core(slot, block):
        return remote(got.at[block], got.at[block], g_core.at[slot], g_recv.at[block], other_core)

    def gather_to_y(n, block):
        return remote(got.at[block], got.at[block], g_y.at[n], g_recv.at[block], other_y)

    def gather_along(sem, block, peer):
        return remote(got.at[block], got.at[block], g_z.at[sem], g_recv.at[block], peer)

    def arrived(block):
        remote(got.at[block], got.at[block], g_core.at[0], g_recv.at[block], other_core).wait_recv()

    def along_z(n, action):
        source = column(n)
        block = at(source, y, c)

        @pl.when(jnp.logical_and(source <= z, z < 3))
        def _():
            action(gather_along(n, block, right))

        @pl.when(jnp.logical_and(source >= z, z > 0))
        def _():
            action(gather_along(n if n else 4, block, left))

    def start(copy):
        copy.start()

    def sent(copy):
        copy.wait_send()

    along_z(0, start)
    gather_to_y(0, me).start()
    gather_to_core(0, me).start()
    gains = got[me, tokens:, :].astype(F32)
    attention = Attention(got if backward else mats, proj, ctx, x_ref, gains[choices:choices + 1], gains[choices + 1:choices + 2], head_dim)
    weights = attention.copies(wq_ref, wk_ref, wv_ref, wo_ref, att_sem)
    if not backward:
        for copy in weights:
            copy.start()

    def pass_on(n):
        block = at(column(n), y, c)
        arrived(block)
        along_z(n, start)
        gather_to_y(n, block).start()
        gather_to_core(n, block).start()

    def order(step):
        late = lax.div(step, 4)
        return step + late * (7 - 2 * step), late

    def pair_base(step):
        n, across = order(step)
        return at(column(n), lax.rem(y + across, 2), 0)

    if backward:
        slots = saved.shape[2] // 2

        def load_saved(step):
            start = pl.multiple_of(pair_base(step) * slots, 2 * slots)
            which = lax.rem(step, 2)
            return pltpu.make_async_copy(u_ref.at[:, pl.ds(start, 2 * slots), :], saved.at[which], load_sem.at[which])

        load_saved(0).start()
        acc1[...] = jnp.zeros_like(acc1)
        acc2[...] = jnp.zeros_like(acc2)
        acc3[...] = jnp.zeros_like(acc3)
    else:
        slots = tokens // 2

    slot_row = lax.broadcasted_iota(jnp.int32, (slots, tokens), 0).astype(F32)

    def masks(block):
        facts = got[block, tokens:, :].astype(F32)
        ids, slot_ids, gates = (facts[:choices, i * tokens:(i + 1) * tokens] for i in range(3))
        plain, gated = [], []
        for e in range(half):
            kept = jnp.logical_and(ids == (me * half + e).astype(F32), slot_ids >= 0.0)
            slot = jnp.sum(jnp.where(kept, slot_ids + 1.0, 0.0), axis=0, keepdims=True) - 1.0
            gate = jnp.sum(jnp.where(kept, gates, 0.0), axis=0, keepdims=True)
            hit = slot == slot_row
            plain.append(jnp.where(hit, 1.0, 0.0).astype(BF16))
            gated.append(jnp.where(hit, gate, 0.0).astype(BF16))
        return jnp.concatenate(plain, axis=0), jnp.concatenate(gated, axis=0)

    def experts_forward(mine, theirs):
        marks = [masks(block) for block in (mine, theirs)]
        placed = [mm(marks[s][0], got[block, :tokens, :]).astype(BF16) for s, block in enumerate((mine, theirs))]
        outs = []
        for e in range(half):
            rows = jnp.concatenate([part[e * slots:(e + 1) * slots] for part in placed], axis=0)
            act_1 = mm(rows, w1_ref[e]).astype(BF16).astype(F32)
            act_3 = mm(rows, w3_ref[e]).astype(BF16).astype(F32)
            hidden = (act_1 * jax.nn.sigmoid(act_1) * act_3).astype(BF16)
            outs.append(mm(hidden, w2_ref[e]).astype(BF16))

        def combine(s):
            return mm_tn(marks[s][1], jnp.concatenate([out[s * slots:(s + 1) * slots] for out in outs], axis=0))

        return combine

    def experts_backward(mine, theirs, which):
        marks = [masks(block) for block in (mine, theirs)]
        placed = [mm(marks[s][1], got[block, :tokens, :]).astype(BF16) for s, block in enumerate((mine, theirs))]
        outs = []
        for e in range(half):
            rows = saved[which, e]
            d_out = jnp.concatenate([part[e * slots:(e + 1) * slots] for part in placed], axis=0)
            pre_1 = mm(rows, w1_ref[e]).astype(BF16).astype(F32)
            pre_3 = mm(rows, w3_ref[e]).astype(BF16).astype(F32)
            sigma = jax.nn.sigmoid(pre_1)
            silu_1 = pre_1 * sigma
            hidden = (silu_1 * pre_3).astype(BF16)
            acc2[e] += mm_tn(hidden, d_out)
            grad_hid = mm_nt(d_out, w2_ref[e]).astype(BF16).astype(F32)
            grad_a1 = (grad_hid * pre_3 * sigma * (1.0 + pre_1 * (1.0 - sigma))).astype(BF16)
            grad_a3 = (grad_hid * silu_1).astype(BF16)
            acc1[e] += mm_tn(rows, grad_a1)
            acc3[e] += mm_tn(rows, grad_a3)
            outs.append((mm_nt(grad_a1, w1_ref[e]) + mm_nt(grad_a3, w3_ref[e])).astype(BF16))

        def combine(s):
            return mm_tn(marks[s][0], jnp.concatenate([out[s * slots:(s + 1) * slots] for out in outs], axis=0))

        return combine

    def send_core(step):
        which = lax.rem(step, 2)
        return remote(stage.at[which], from_core.at[which], s_core.at[which], r_core.at[which], other_core)

    def send_y(n):
        return remote(own.at[4 + n, :, first], from_y.at[n], s_y.at[n], r_y.at[n], other_y)

    def take_y(n):
        send_y(n).wait_recv()
        own[n, :, :main] += from_y[n]

    def hop(n, source, landing, base, send, recv, action):
        goal = column(n)

        @pl.when(goal > z)
        def _():
            action(remote(source, landing.at[base + goal], send, recv.at[base + goal], right))

        @pl.when(goal == z - 1)
        def _():
            action(remote(source, landing.at[base + 4], send, recv.at[base + 4], left))

        @pl.when(goal < z - 1)
        def _():
            action(remote(source, landing.at[base + goal], send, recv.at[base + goal], left))

    def chain(n, action):
        hop(n, own.at[n, :, first], from_z, 0, s_z.at[n - 1], r_z, action)

    def take_z(n, slot):
        remote(own.at[n, :, first], from_z.at[slot], s_z.at[0], r_z.at[slot], left).wait_recv()
        own[n, :, :main] += from_z[slot]

    def side_chain(across, n, action):
        hop(n, own.at[4 * across + n, :, last], side_z, 5 * across, sz_send.at[3 * across + n - 1], sz_recv, action)

    def side_take(across, n, slot):
        at_slot = 5 * across + slot
        remote(own.at[n, :, last], side_z.at[at_slot], sz_send.at[0], sz_recv.at[at_slot], left).wait_recv()
        own[4 * across + n, :, main:] += side_z[at_slot]

    def side_cross():
        return remote(own.at[4, :, last], side_y, sy_send, sy_recv, other_y)

    def at_steps(step, who, table, action):
        for when, across, n in table:
            @pl.when(jnp.logical_and(who, step == when))
            def _():
                action(across, n)

    def side_join(across, n):
        side_take(across, n, column(n))
        side_chain(across, n, start)

    def side_gather(across):
        @pl.when(z > 0)
        def _():
            side_take(across, 0, z)

        @pl.when(z < 3)
        def _():
            side_take(across, 0, 4)

    def step_body(step, carry):
        n, across = order(step)
        base = pair_base(step)
        which = lax.rem(step, 2)

        @pl.when(step == 1)
        def _():
            pass_on(1)

        @pl.when(jnp.logical_or(jnp.logical_and(step == 1, inside), jnp.logical_and(step == 2, at_end)))
        def _():
            pass_on(2)

        @pl.when(jnp.logical_or(jnp.logical_and(step == 2, inside), jnp.logical_and(step == 3, at_end)))
        def _():
            pass_on(3)

        @pl.when(jnp.logical_and(step >= 1, step <= 4))
        def _():
            block = at(column(step - 1), 1 - y, c)
            arrived(block)
            gather_to_core(3 + step, block).start()

        arrived(base + 1 - c)
        if backward:
            @pl.when(step < 7)
            def _():
                load_saved(step + 1).start()
            load_saved(step).wait()
            low, high = base, base + 1
            combine = experts_backward(low, high, which)
        else:
            low, high = base, base + 1
            combine = experts_forward(low, high)

        @pl.when(step >= 2)
        def _():
            send_core(step).wait_send()

        first, second = combine(0), combine(1)

        @pl.when(c == 0)
        def _():
            stage[which] = second
            own[across * 4 + n] = first

        @pl.when(c == 1)
        def _():
            stage[which] = first
            own[across * 4 + n] = second

        send_core(step).start()

        send_core(step).wait_recv()
        own[across * 4 + n] += from_core[which]

        @pl.when(across == 1)
        def _():
            send_y(n).start()

        at_steps(step, at_end, ((1, 0, 1), (2, 0, 2), (3, 0, 3), (4, 1, 3), (5, 1, 2), (6, 1, 1)), lambda across, n: side_chain(across, n, start))
        at_steps(step, inside, ((4, 0, 2), (5, 0, 3), (6, 0, 1), (6, 1, 3), (7, 1, 2), (7, 1, 1)), side_join)

        if not backward:
            @pl.when(step == 1)
            def _():
                attention.heads()

            @pl.when(step == 2)
            def _():
                pull_output()

        @pl.when(step == 6)
        def _():
            take_y(3)

            @pl.when(at_end)
            def _():
                chain(3, start)

        return carry

    def pull_output():
        hid = attention.hidden()
        d_norm, gn2_ref[...] = attention.norm_pull(hid.astype(F32), attention.gain_2, du_ref[...].astype(F32))
        d_hid = (dy_ref[...].astype(F32) + d_norm.astype(F32)).astype(BF16)
        dx_ref[...] = d_hid
        for i in range(4):
            d_ctx[:, i * attention.chunk:(i + 1) * attention.chunk] = mm_nt(d_hid, attention.weight(4 + i)).astype(BF16)
        for i in range(4):
            go_ref[pl.ds(i * attention.chunk, attention.chunk), :] = mm_tn(attention.part(ctx[...], i), d_hid).astype(BF16)

    if not backward:
        for copy in weights:
            copy.wait()
        attention.project()
    lax.fori_loop(0, 8, step_body, 0)
    if backward:
        stores = [pltpu.make_async_copy(acc, ref, store_sem.at[i]) for i, (acc, ref) in enumerate(((acc1, gw1_ref), (acc2, gw2_ref), (acc3, gw3_ref)))]
        for store in stores:
            store.start()

    for n in range(4):
        along_z(n, sent)
        gather_to_y(n, me).wait_send()
    for slot in range(8):
        gather_to_core(slot, me).wait_send()
    if backward:
        for copy in weights:
            copy.start()

    def join(n):
        @pl.when(inside)
        def _():
            take_z(n, column(n))
            chain(n, start)

    def pass_sum(n):
        take_y(n)

        @pl.when(at_end)
        def _():
            chain(n, start)

    join(3)
    pass_sum(2)
    if backward:
        for copy in weights:
            copy.wait()
        attention.project()
        attention.heads()
    else:
        attention.pull_heads(d_ctx, d_proj)
    join(2)
    side_gather(1)
    side_cross().start()
    pass_sum(1)
    kv = attention.kv
    if backward:
        hid = attention.hidden()
        h_ref[...] = hid
        norm_ref[...] = attention.norm(hid.astype(F32), attention.gain_2)
    else:
        rows = attention.normed()
        for i in range(4):
            block = pl.ds(i * attention.chunk, attention.chunk)
            gq_ref[block, :] = mm_tn(attention.part(rows, i), d_proj[:, :dim]).astype(BF16)
            gk_ref[block, :] = mm_tn(attention.part(rows, i), d_proj[:, dim:dim + kv]).astype(BF16)
            gv_ref[block, :] = mm_tn(attention.part(rows, i), d_proj[:, dim + kv:]).astype(BF16)
    join(1)
    if not backward:
        pulled = [mm_nt(d_proj[:, :dim], attention.weight(i)) + mm_nt(d_proj[:, dim:], attention.weight(8 + i)) for i in range(4)]
        d_rows = jnp.concatenate(pulled, axis=1).astype(BF16).astype(F32)
        d_x, gn1_ref[...] = attention.norm_pull(x_ref[...].astype(F32), attention.gain_1, d_rows)
        dx_ref[...] = (dx_ref[...].astype(F32) + d_x.astype(F32)).astype(BF16)
    side_gather(0)
    take_y(0)
    side_cross().wait_recv()
    own[0, :, main:] += side_y[...]

    @pl.when(z > 0)
    def _():
        take_z(0, z)

    @pl.when(z < 3)
    def _():
        take_z(0, 4)

    total = own[0] if backward else base_ref[...].astype(F32) + own[0]
    out_ref[...] = total.astype(BF16)
    for n in (3, 2, 1):
        chain(n, sent)
        side_chain(0, n, sent)
        side_chain(1, n, sent)
    side_cross().wait_send()
    for n in range(4):
        send_y(n).wait_send()
    send_core(0).wait_send()
    send_core(1).wait_send()
    if backward:
        for store in stores:
            store.wait()


def exchange(backward, rows, weights, tokens, head_dim, choices, sequence, saved=None):
    w_1, w_3, w_2 = weights
    dim = rows.shape[1]
    half, ff = w_1.shape[0], w_1.shape[2]
    dma = pltpu.SemaphoreType.DMA
    block = (tokens, dim)
    model = (dim, dim)
    narrow = (dim, dim // 2)
    scratch = [
        pltpu.VMEM((tokens, 2 * dim), BF16),
        pltpu.VMEM(block, BF16),
        dma((16,)),
    ]
    if not backward:
        scratch += [pltpu.VMEM(block, BF16), pltpu.VMEM((tokens, 2 * dim), BF16), pltpu.VMEM((12, dim // 4, dim), BF16)]
    scratch += [
        pltpu.VMEM((16,) + rows.shape, BF16),
        pltpu.VMEM((8,) + block, F32),
        pltpu.VMEM((2,) + block, F32),
        pltpu.VMEM((2,) + block, F32),
        pltpu.VMEM((4, tokens, dim - dim // SIDE), F32),
        pltpu.VMEM((5, tokens, dim - dim // SIDE), F32),
    ]
    tail = [pltpu.VMEM((10, tokens, dim // SIDE), F32), pltpu.VMEM((tokens, dim // SIDE), F32), dma((6,)), dma((10,)), dma(()), dma(()), dma((16,)), dma((8,)), dma((4,)), dma((5,)), dma((2,)), dma((2,)), dma((4,)), dma((4,)), dma((3,)), dma((5,))]
    any_spec = pl.BlockSpec(memory_space=pl.ANY)
    vmem_spec = pl.BlockSpec(memory_space=pltpu.VMEM)
    if backward:
        slots = saved.shape[1] // 16
        scratch += [
            pltpu.VMEM((2, half, 2 * slots, dim), BF16),
            pltpu.VMEM((half, dim, ff), F32),
            pltpu.VMEM((half, ff, dim), F32),
            pltpu.VMEM((half, dim, ff), F32),
            dma(()), dma((2,)), dma((3,)),
        ]
        operands = (rows, saved, w_1, w_3, w_2) + sequence
        in_specs = [any_spec, any_spec] + [vmem_spec] * 4 + [any_spec] * 4
        out_shape = [jax.ShapeDtypeStruct(block, BF16), jax.ShapeDtypeStruct((half, dim, ff), F32), jax.ShapeDtypeStruct((half, ff, dim), F32), jax.ShapeDtypeStruct((half, dim, ff), F32), jax.ShapeDtypeStruct(block, BF16), jax.ShapeDtypeStruct(block, BF16)]
        out_specs = [vmem_spec, any_spec, any_spec, any_spec, vmem_spec, vmem_spec]
    else:
        scratch += [dma(())]
        operands = (rows, w_1, w_3, w_2) + sequence
        in_specs = [any_spec] + [vmem_spec] * 4 + [any_spec] * 4 + [vmem_spec] * 3
        out_shape = [jax.ShapeDtypeStruct(block, BF16)] * 2
        out_shape += [jax.ShapeDtypeStruct(shape, BF16) for shape in (model, narrow, narrow, model)]
        out_shape += [jax.ShapeDtypeStruct((1, dim), F32)] * 2
        out_specs = [vmem_spec] * 8
    return pl.pallas_call(
        functools.partial(exchange_kernel, backward, head_dim, choices),
        out_shape=out_shape,
        in_specs=in_specs,
        out_specs=out_specs,
        scratch_shapes=scratch + tail,
        name='exchange_b' if backward else 'exchange_a',
        compiler_params=pltpu.CompilerParams(collective_id=1 if backward else 0, has_side_effects=True, vmem_limit_bytes=VMEM_BYTES),
    )(*operands)


def solution(mesh):
    group = mesh.shape['expert']

    def local_step(x_a, x_b, dy_b, eid_a, slot_a, gate_a, eid_b, slot_b, gate_b, u_b, norm_1, norm_2, w_q, w_k, w_v, w_o, w_1, w_2, w_3):
        local_experts = w_1.shape[0]
        model_dim = x_a.shape[1]

        tokens = x_a.shape[0]

        def with_routing(rows, expert_ids, slot_ids, gates):
            facts = jnp.concatenate([array.astype(jnp.bfloat16).T for array in (expert_ids, slot_ids, gates)], axis=1)
            facts = jnp.pad(facts, ((0, 0), (0, model_dim - facts.shape[1])))
            table = jnp.concatenate([facts, norm_1[None], norm_2[None]], axis=0)
            table = jnp.pad(table, ((0, 16 - table.shape[0]), (0, 0)))
            return jnp.concatenate([rows, table], axis=0)

        weights = (w_1, w_3, w_2)
        head_dim = w_q.shape[2]
        layer = (w_q.reshape(model_dim, -1), w_k.reshape(model_dim, -1), w_v.reshape(model_dim, -1), w_o.reshape(-1, model_dim))
        du_rows, grad_w1, grad_w2, grad_w3, h_a, u_a = exchange(True, with_routing(dy_b, eid_b, slot_b, gate_b), weights, tokens, head_dim, eid_b.shape[1], (x_a,) + layer, u_b)
        y_a, dx_b, g_q, g_k, g_v, g_o, g_n1, g_n2 = exchange(False, with_routing(u_a, eid_a, slot_a, gate_a), weights, tokens, head_dim, eid_a.shape[1], (x_b,) + layer + (dy_b, du_rows, h_a))
        g_q, g_k, g_v, g_o = (grad.astype(jnp.float32).reshape(weight.shape) for grad, weight in ((g_q, w_q), (g_k, w_k), (g_v, w_v), (g_o, w_o)))
        g_n1, g_n2 = g_n1[0], g_n2[0]
        return (y_a, dx_b, grad_w1, grad_w2, grad_w3, g_q[None], g_k[None], g_v[None], g_o[None], g_n1[None], g_n2[None])

    row_spec = P(('data', 'expert'), None)
    cube_spec = P(('data', 'expert'), None, None)
    quad_spec = P(('data', 'expert'), None, None, None)
    expert_spec = P('expert', None, None)
    in_specs = (row_spec, row_spec, row_spec, row_spec, row_spec, row_spec, row_spec, row_spec, row_spec, cube_spec, P(), P(), P(), P(), P(), P(), expert_spec, expert_spec, expert_spec)
    out_specs = (row_spec, row_spec, cube_spec, cube_spec, cube_spec, quad_spec, quad_spec, quad_spec, quad_spec, row_spec, row_spec)
    return jax.shard_map(local_step, mesh=mesh, in_specs=in_specs, out_specs=out_specs, check_vma=False)
```
